32 devices in a mesh: dp: 4 (over x, core), table: 8 (over z, y).
Axes of the slice: x: 2, y: 2, z: 4, core: 2. Of those that a mesh axis runs over, the one named last changes fastest.
Arguments:
- out_grad: bfloat16 [32768, 1024], P(('dp', 'table')), may hold values from -0.1875 to 0.1875
- pair_cells: int32 [32768, 8, 32], P(('dp', 'table')), may hold values from 0 to 4095
- weight_codes: int32 [32768, 8, 32], P(('dp', 'table')), may hold values from -127 to 127
- head_scale: float32 [8], replicated, may hold values from 0.5 to 2
- touch_slots: int32 [8, 8, 4], replicated, may hold values from 0 to 7
Outputs:
- grad_rows: bfloat16 [8192, 1024], P('table', 'dp')
The draws below stay inside these ranges and needn't reach their ends.
All inputs are finite; a program needn't handle non-finite values.
Results may differ from the reference program's by a relative error of at most 0.0098.
Values may be sent and summed in bfloat16 or wider, within the bound.
No kernel may reach another device: no remote copies, remote signals or barrier semaphores. Data moves between devices by JAX's collectives and lax.ppermute only.
A program may use at most 128 MiB of HBM per device.

```python
import math
import jax
import jax.numpy as jnp
from jax import lax

V = 1024
HEADS = 8
TOPK = 32
ROWS = 128
TOUCH = 32
OWN = 8
TOK_DEV = 1024
CAP = 4
TOKENS = 32768
N_DP = 4
N_TABLE = 8


def set_ends(result, key, low, top_value):
    spot = [jax.random.randint(jax.random.fold_in(key, axis), (), 0, length) for axis, length in enumerate(result.shape)]
    longest = result.shape.index(max(result.shape))
    beside = spot[:longest] + [(spot[longest] + 1) % result.shape[longest]] + spot[longest + 1:]
    return result.at[tuple(spot)].set(low).at[tuple(beside)].set(top_value)


def level_of(own_key, shape, shards, least, largest):
    def one(axis_at, shards_of):
        draws = jax.random.uniform(jax.random.fold_in(jax.random.fold_in(own_key, 6), axis_at), (shards_of,), jnp.float32, least / len(shards), largest / len(shards))
        return jnp.repeat(jnp.exp(draws), shape[axis_at] // shards_of).reshape((-1,) + (1,) * (len(shape) - axis_at - 1))

    loudness = one(*shards[0])
    for cut in shards[1:]:
        loudness = loudness * one(*cut)
    return loudness


def gaussian(own_key, extent, spread, reach, shards=(), held_as=jnp.bfloat16):
    drawn = jax.random.normal(own_key, extent, jnp.float32) * spread
    if len(shards) > 0:
        drawn = level_of(own_key, extent, shards, -0.22, 0.18) * drawn
    return jnp.clip(drawn, min=-reach, max=reach).astype(held_as)


def setup_inputs(seed: int = 0) -> dict:
    keys = jax.random.split(jax.random.key(seed), 6)
    out_grad = gaussian(keys[0], (TOKENS, V), ((ROWS * OWN) ** 0.5 / (N_DP * TOK_DEV * HEADS * TOPK) ** 0.5), 0.1875, ((0, 32),))
    pair_cells = set_ends(jax.random.randint(keys[1], (TOKENS, HEADS, TOPK), 0, TOUCH * ROWS), jax.random.fold_in(keys[1], 1), 0, (TOUCH * ROWS) - 1).astype(jnp.int32)
    weight_codes = set_ends(jax.random.randint(keys[2], (TOKENS, HEADS, TOPK), -127, 128), jax.random.fold_in(keys[2], 1), -127, 127).astype(jnp.int32)
    head_scale = jnp.clip(jnp.exp(jax.random.uniform(keys[3], (HEADS,), jnp.float32, math.log(0.5), math.log(2.0))), 0.5, 2.0)
    touch_slots = set_ends(jax.random.randint(keys[4], (N_TABLE, N_TABLE, CAP), 0, OWN), jax.random.fold_in(keys[4], 1), 0, OWN - 1).astype(jnp.int32)
    return {"out_grad": out_grad, "pair_cells": pair_cells, "weight_codes": weight_codes, "head_scale": head_scale, "touch_slots": touch_slots}


def reference(out_grad, pair_cells, weight_codes, head_scale, touch_slots):
    devices = N_DP * N_TABLE
    weight = weight_codes.astype(jnp.float32) * head_scale[None, :, None].astype(jnp.float32) / 128.0
    cells = pair_cells.reshape(devices, TOK_DEV, HEADS * TOPK)
    weights = weight.reshape(devices, TOK_DEV, HEADS * TOPK)
    grads = out_grad.reshape(devices, TOK_DEV, V).astype(jnp.float32)
    tok_iota = jnp.arange(TOK_DEV, dtype=jnp.int32)
    cap = TOUCH // N_TABLE

    def one(total, index):
        group = index % N_TABLE
        coef = jnp.zeros((TOUCH * ROWS, TOK_DEV), jnp.float32)
        coef = coef.at[cells[index], tok_iota[:, None]].add(weights[index])
        coef = lax.optimization_barrier(coef.astype(jnp.bfloat16)).astype(jnp.float32)
        partial_value = jnp.dot(coef, grads[index], precision=lax.Precision.HIGHEST)
        owners = jnp.arange(N_TABLE, dtype=jnp.int32)[:, None] * OWN
        target = (owners + touch_slots[group].astype(jnp.int32)).reshape(N_TABLE * cap)
        total = total.at[target].add(partial_value.reshape(TOUCH, ROWS, V))
        return total, None

    start = jnp.zeros((N_TABLE * OWN, ROWS, V), jnp.float32)
    total, _ = lax.scan(one, start, jnp.arange(devices, dtype=jnp.int32))
    return total.reshape(N_TABLE * OWN * ROWS, V).astype(jnp.bfloat16)
```

```python
import functools

import jax
import jax.numpy as jnp
from jax import lax
from jax.experimental import pallas as pl
from jax.experimental.pallas import tpu as pltpu
from jax.sharding import PartitionSpec as P

ROWS = 128
TOUCH = 32
OWN = 8
CELL_BITS = 12
CODE_BIAS = 128
BLOCK = 128


def coef_kernel(packed_ref, scale_ref, out_ref, low_ref, high_ref, weight_ref, table_ref, *, capacity):
    block, pairs = packed_ref.shape
    groups = TOUCH // capacity
    packed = packed_ref[...]
    cell = packed & ((1 << CELL_BITS) - 1)
    low_ref[...] = (cell % ROWS).astype(jnp.float32)
    high_ref[...] = (cell // ROWS).astype(jnp.float32)
    weight_ref[...] = ((packed >> CELL_BITS) - CODE_BIAS).astype(jnp.float32) * scale_ref[...]
    row_iota = lax.broadcasted_iota(jnp.int32, (ROWS, pairs), 0).astype(jnp.float32).astype(jnp.bfloat16)
    tile_iota = lax.broadcasted_iota(jnp.int32, (TOUCH, pairs), 0).astype(jnp.float32).astype(jnp.bfloat16)

    def spread(ref, token, count):
        row = jnp.broadcast_to(ref[pl.ds(token, 1), :], (16, pairs)).astype(jnp.bfloat16)
        return jnp.concatenate([row] * (count // 16), axis=0)

    def one(token):
        low = spread(low_ref, token, ROWS)
        row_hot = jnp.where(low == row_iota, jnp.bfloat16(1), jnp.bfloat16(0))
        high = spread(high_ref, token, TOUCH)
        weight = spread(weight_ref, token, TOUCH)
        tile_hot = jnp.where(high == tile_iota, weight, jnp.bfloat16(0))
        table = lax.dot_general(
            tile_hot, row_hot, (((1,), (1,)), ((), ())), preferred_element_type=jnp.float32
        )
        table_ref[pl.ds(token, TOUCH, stride=block), :] = table

    unroll = 8

    @pl.loop(0, block // unroll)
    def _(step):
        for i in range(unroll):
            one(step * unroll + i)

    for j in range(TOUCH):
        place = (j % capacity) * groups + j // capacity
        part = table_ref[pl.ds(j * block, block), :]
        out_ref[pl.ds(place * ROWS, ROWS), :] = part.T.astype(jnp.bfloat16)


def coef_table(packed, scale, capacity):
    tokens, pairs = packed.shape
    return pl.pallas_call(
        functools.partial(coef_kernel, capacity=capacity),
        grid=(tokens // BLOCK,),
        in_specs=[
            pl.BlockSpec((BLOCK, pairs), lambda i: (i, 0)),
            pl.BlockSpec((1, pairs), lambda i: (0, 0)),
        ],
        out_specs=pl.BlockSpec((TOUCH * ROWS, BLOCK), lambda i: (0, i)),
        out_shape=jax.ShapeDtypeStruct((TOUCH * ROWS, tokens), jnp.bfloat16),
        scratch_shapes=[
            pltpu.VMEM((BLOCK, pairs), jnp.float32),
            pltpu.VMEM((BLOCK, pairs), jnp.float32),
            pltpu.VMEM((BLOCK, pairs), jnp.float32),
            pltpu.VMEM((TOUCH * BLOCK, ROWS), jnp.float32),
        ],
        cost_estimate=pl.CostEstimate(
            flops=2 * tokens * pairs * TOUCH * ROWS * 4, transcendentals=0, bytes_accessed=tokens * (pairs * 4 + TOUCH * ROWS * 2)
        ),
        name="coef_table",
    )(packed, scale)


def part_kernel(pick_ref, coef_ref, *refs):
    count = len(refs) // 2
    coef = coef_ref[...]
    for grad_ref, out_ref in zip(refs[:count], refs[count:]):
        out_ref[...] = jnp.dot(coef, grad_ref[...], preferred_element_type=jnp.float32).astype(jnp.bfloat16)


def partials(coef, grads, picks, width, chunk, chunks):
    tokens = coef.shape[1]
    span = coef.shape[0] // chunks
    rows = min(span, 512)
    steps = span // rows
    count = picks.shape[0]
    base = chunk * steps
    return pl.pallas_call(
        part_kernel,
        grid_spec=pltpu.PrefetchScalarGridSpec(
            num_scalar_prefetch=1,
            grid=(steps,),
            in_specs=[pl.BlockSpec((rows, tokens), lambda i, pick: (base + i, 0))]
            + [pl.BlockSpec((tokens, width), lambda i, pick, n=n: (0, pick[n])) for n in range(count)],
            out_specs=[pl.BlockSpec((rows, width), lambda i, pick: (i, 0)) for _ in range(count)],
        ),
        out_shape=[jax.ShapeDtypeStruct((span, width), jnp.bfloat16) for _ in range(count)],
        cost_estimate=pl.CostEstimate(
            flops=2 * tokens * span * width * count,
            transcendentals=0,
            bytes_accessed=2 * (tokens * span + count * width * (tokens + span)),
        ),
        name="partials",
    )(picks, coef, *([grads] * count))


def gather_kernel(slot_ref, *refs):
    out_ref, sum_ref = refs[-2:]
    sum_ref[...] = jnp.zeros(sum_ref.shape, jnp.float32)
    for k, part_ref in enumerate(refs[:-2]):
        for g in range(part_ref.shape[0]):
            slot = slot_ref[g, k]
            sum_ref[slot] += part_ref[g].astype(jnp.float32)
    out_ref[...] = sum_ref[...].astype(jnp.bfloat16)


def gather_tiles(slots, parts):
    width = parts[0].shape[2]
    return pl.pallas_call(
        gather_kernel,
        grid_spec=pltpu.PrefetchScalarGridSpec(
            num_scalar_prefetch=1,
            grid=(1,),
            in_specs=[pl.BlockSpec(p.shape, lambda i, slot: (0, 0, 0)) for p in parts],
            out_specs=pl.BlockSpec((OWN, ROWS, width), lambda i, slot: (0, 0, 0)),
            scratch_shapes=[pltpu.VMEM((OWN, ROWS, width), jnp.float32)],
        ),
        out_shape=jax.ShapeDtypeStruct((OWN, ROWS, width), jnp.bfloat16),
        name="gather_tiles",
    )(slots, *parts)


def body(out_grad, pair_cells, weight_codes, head_scale, touch_slots, *, replicas):
    tokens, value = out_grad.shape
    width = value // replicas
    groups = touch_slots.shape[0]
    capacity = touch_slots.shape[2]
    heads, slots = pair_cells.shape[1:]
    pairs = heads * slots
    replica = lax.axis_index("dp")
    owner = lax.axis_index("table")
    packed = (pair_cells | ((weight_codes + CODE_BIAS) << CELL_BITS)).reshape(tokens, pairs)
    scale = jnp.repeat(head_scale / 128.0, slots).reshape(1, pairs)
    coef = coef_table(packed, scale, capacity)

    def swap(array, bit):
        return lax.ppermute(array, "dp", [(i, i ^ bit) for i in range(replicas)])

    def add(*arrays):
        total = arrays[0].astype(jnp.float32)
        for array in arrays[1:]:
            total = total + array.astype(jnp.float32)
        return total.astype(jnp.bfloat16)

    half = replicas // 2
    far = [half + m for m in range(half)]
    near = list(range(half))
    pick = lambda masks: jnp.stack([replica ^ m for m in masks]).astype(jnp.int32)
    held = [dict() for _ in range(capacity)]
    for masks in (far, near):
        for chunk in range(capacity):
            outs = partials(coef, out_grad, pick(masks), width, chunk, capacity)
            held[chunk].update(zip(masks, outs))
    parts = []
    for chunk in range(capacity):
        piece = {m: [a] for m, a in held[chunk].items()}
        bit = 1
        while bit < replicas:
            for m in sorted(piece, reverse=True):
                if m & bit:
                    terms = piece.pop(m)
                    sent = terms[0] if len(terms) == 1 else add(*terms)
                    piece[m ^ bit].append(swap(sent, bit))
            bit *= 2
        mine = add(*piece[0]).reshape(groups, ROWS, width)
        parts.append(lax.all_to_all(mine, "table", split_axis=0, concat_axis=0, tiled=True))
    mine_slots = lax.dynamic_index_in_dim(touch_slots, owner, 1, keepdims=False)
    return gather_tiles(mine_slots, parts).reshape(OWN * ROWS, width)


def solution(mesh):
    return jax.shard_map(
        functools.partial(body, replicas=mesh.shape["dp"]),
        mesh=mesh,
        in_specs=(
            P(("dp", "table"), None),
            P(("dp", "table"), None, None),
            P(("dp", "table"), None, None),
            P(),
            P(),
        ),
        out_specs=P("table", "dp"),
        check_vma=False,
    )
```

```python
import functools

import jax
import jax.numpy as jnp
from jax import lax
from jax.experimental import pallas as pl
from jax.experimental.pallas import tpu as pltpu
from jax.sharding import PartitionSpec as P

ROWS = 128
TOUCH = 32
OWN = 8
CELL_BITS = 12
CODE_BIAS = 128
BLOCK = 128
SIDE = 64
CHUNKS = 8


def coef_kernel(scale_ref, cells_ref, codes_ref, out_ref, low_ref, high_ref, weight_ref, table_ref):
    block = out_ref.shape[0]
    heads = scale_ref.shape[0]
    packed = (cells_ref[...] | ((codes_ref[...] + CODE_BIAS) << CELL_BITS)).T
    pairs = packed.shape[1]
    stride = table_ref.shape[0] // TOUCH
    tile = (packed >> 7) & (TOUCH - 1)
    upper = (packed >> 6) & 1
    low_ref[...] = (packed & (SIDE - 1)).astype(jnp.float32)
    high_ref[...] = (tile + TOUCH * upper).astype(jnp.float32)
    head = lax.broadcasted_iota(jnp.int32, (1, pairs), 1) // (pairs // heads)
    scale = jnp.zeros((1, pairs), jnp.float32)
    for h in range(heads):
        scale = jnp.where(head == h, scale_ref[h] / 128.0, scale)
    weight_ref[...] = ((packed >> CELL_BITS) - CODE_BIAS).astype(jnp.float32) * scale
    iota = lax.broadcasted_iota(jnp.int32, (SIDE, pairs), 0).astype(jnp.float32).astype(jnp.bfloat16)

    def spread(ref, token):
        row = jnp.broadcast_to(ref[pl.ds(token, 1), :], (16, pairs)).astype(jnp.bfloat16)
        return jnp.concatenate([row] * (SIDE // 16), axis=0)

    for token in range(block):
        low_hot = jnp.where(spread(low_ref, token) == iota, jnp.bfloat16(1), jnp.bfloat16(0))
        high_hot = jnp.where(spread(high_ref, token) == iota, spread(weight_ref, token), jnp.bfloat16(0))
        table = lax.dot_general(
            high_hot, low_hot, (((1,), (1,)), ((), ())), preferred_element_type=jnp.float32
        )
        table = jnp.concatenate([table[:TOUCH], table[TOUCH:]], axis=1)
        table_ref[pl.ds(token, TOUCH, stride=stride), :] = table
    for j in range(TOUCH):
        out_ref[:, j * ROWS : (j + 1) * ROWS] = table_ref[pl.ds(j * stride, block), :].astype(jnp.bfloat16)


def coef_table(head_scale, cells, codes):
    pairs, tokens = cells.shape
    spec = pl.BlockSpec((pairs, BLOCK), lambda i, scale: (0, i))
    return pl.pallas_call(
        coef_kernel,
        grid_spec=pltpu.PrefetchScalarGridSpec(
            num_scalar_prefetch=1,
            grid=(tokens // BLOCK,),
            in_specs=[spec, spec],
            out_specs=pl.BlockSpec((BLOCK, TOUCH * ROWS), lambda i, scale: (i, 0)),
            scratch_shapes=[
                pltpu.VMEM((BLOCK, pairs), jnp.float32),
                pltpu.VMEM((BLOCK, pairs), jnp.float32),
                pltpu.VMEM((BLOCK, pairs), jnp.float32),
                pltpu.VMEM((TOUCH * (BLOCK + 8), ROWS), jnp.float32),
            ],
        ),
        out_shape=jax.ShapeDtypeStruct((tokens, TOUCH * ROWS), jnp.bfloat16),
        cost_estimate=pl.CostEstimate(
            flops=2 * tokens * pairs * TOUCH * ROWS * 4,
            transcendentals=0,
            bytes_accessed=tokens * (pairs * 8 + TOUCH * ROWS * 2),
        ),
        name="coef_table",
    )(head_scale, cells, codes)


def part_kernel(place_ref, coef_ref, *refs):
    count = (len(refs) - 1) // 2
    flip_ref = refs[-1]
    width = refs[0].shape[1]

    @pl.when(pl.program_id(0) == 0)
    def _():
        for n in range(count):
            flip_ref[pl.ds(n * width, width), :] = refs[n][...].T

    product = jnp.dot(flip_ref[...], coef_ref[...], preferred_element_type=jnp.float32)
    for n in range(count):
        for c in range(refs[count + n].shape[1]):
            part = product[n * width : (n + 1) * width, c * ROWS : (c + 1) * ROWS]
            refs[count + n][0, c] = part.astype(jnp.bfloat16)


def partials(place, coef, grads, masks, width, capacity, groups, first, length):
    tokens = coef.shape[0]
    count = len(masks)
    return pl.pallas_call(
        part_kernel,
        grid_spec=pltpu.PrefetchScalarGridSpec(
            num_scalar_prefetch=1,
            grid=(length,),
            in_specs=[
                pl.BlockSpec((tokens, capacity * ROWS), lambda i, place: (0, place[1] ^ (groups - 1 - first - i)))
            ]
            + [pl.BlockSpec((tokens, width), lambda i, place, m=m: (0, place[0] ^ m)) for m in masks],
            out_specs=[
                pl.BlockSpec((1, capacity, width, ROWS), lambda i, place: (i, 0, 0, 0)) for _ in masks
            ],
            scratch_shapes=[pltpu.VMEM((count * width, tokens), jnp.bfloat16)],
        ),
        out_shape=[jax.ShapeDtypeStruct((length, capacity, width, ROWS), jnp.bfloat16) for _ in masks],
        cost_estimate=pl.CostEstimate(
            flops=2 * tokens * length * capacity * ROWS * width * count,
            transcendentals=0,
            bytes_accessed=2 * length * capacity * ROWS * (tokens + count * width) + 2 * count * width * tokens,
        ),
        name="partials",
    )(place, coef, *([grads] * count))


def gather_kernel(place_ref, slot_ref, *refs):
    groups = (len(refs) - 3) // 2
    part_refs, out_ref = refs[:groups], refs[groups]
    buffer_refs, sum_ref, semaphores = refs[groups + 1 : -2], refs[-2], refs[-1]
    capacity = part_refs[0].shape[0]
    owner = place_ref[1]
    copies = [
        pltpu.make_async_copy(part, buffer, semaphores.at[n])
        for n, (part, buffer) in enumerate(zip(part_refs, buffer_refs))
    ]
    for copy in copies:
        copy.start()
    sum_ref[...] = jnp.zeros(sum_ref.shape, jnp.float32)
    for n in range(groups):
        copies[n].wait()
        for c in range(capacity):
            slot = slot_ref[((owner ^ n) * groups + owner) * capacity + c]
            sum_ref[slot] += buffer_refs[n][c].astype(jnp.float32)
    for k in range(OWN):
        out_ref[pl.ds(k * ROWS, ROWS), :] = sum_ref[k].T.astype(jnp.bfloat16)


def gather_tiles(place, slots, parts):
    capacity, width = parts[0].shape[:2]
    return pl.pallas_call(
        gather_kernel,
        grid_spec=pltpu.PrefetchScalarGridSpec(
            num_scalar_prefetch=2,
            grid=(1,),
            in_specs=[pl.BlockSpec(memory_space=pl.ANY) for _ in parts],
            out_specs=pl.BlockSpec((OWN * ROWS, width), lambda i, place, slots: (0, 0)),
            scratch_shapes=[pltpu.VMEM((capacity, width, ROWS), jnp.bfloat16) for _ in parts]
            + [pltpu.VMEM((OWN, width, ROWS), jnp.float32), pltpu.SemaphoreType.DMA((len(parts),))],
        ),
        out_shape=jax.ShapeDtypeStruct((OWN * ROWS, width), jnp.bfloat16),
        name="gather_tiles",
    )(place, slots, *parts)


def add(*arrays):
    total = arrays[0].astype(jnp.float32)
    for array in arrays[1:]:
        total = total + array.astype(jnp.float32)
    return total.astype(jnp.bfloat16)


def body(out_grad, pair_cells, weight_codes, head_scale, touch_slots, *, replicas):
    tokens, value = out_grad.shape
    width = value // replicas
    groups = touch_slots.shape[0]
    capacity = touch_slots.shape[2]
    pairs = pair_cells.shape[1] * pair_cells.shape[2]
    place = jnp.stack([lax.axis_index("dp"), lax.axis_index("table")]).astype(jnp.int32)
    by_pair = lambda array: array.transpose(1, 2, 0).reshape(pairs, tokens)
    coef = coef_table(head_scale, by_pair(pair_cells), by_pair(weight_codes))

    def swap(array, axis, bit):
        return lax.ppermute(array, axis, [(i, i ^ bit) for i in range(lax.axis_size(axis))])

    chunks = min(CHUNKS, groups)
    size = groups // chunks
    half = replicas // 2
    early = max(1, chunks // 4) * size
    pieces = [{m: [] for m in range(0, replicas, 2)} for _ in range(chunks)]
    for masks, first, length in (
        (range(half, replicas), 0, early),
        (range(half, replicas), early, groups - early),
        (range(half), 0, groups),
    ):
        outs = partials(place, coef, out_grad, list(masks), width, capacity, groups, first, length)
        for m, array in zip(masks, outs):
            if m & 1:
                array = swap(array, "dp", 1)
            for start in range(0, length, size):
                pieces[(first + start) // size][m & ~1].append(array[start : start + size])
    parts = {}
    for chunk, piece in enumerate(pieces):
        bit = 2
        while bit < replicas:
            for m in sorted(piece, reverse=True):
                if m & bit:
                    piece[m ^ bit].append(swap(add(*piece.pop(m)), "dp", bit))
            bit *= 2
        mine = add(*piece[0])
        for i in range(size):
            distance = groups - 1 - chunk * size - i
            parts[distance] = swap(mine[i], "table", distance) if distance else mine[i]
    return gather_tiles(place, touch_slots.reshape(-1), [parts[n] for n in range(groups)])


def solution(mesh):
    return jax.shard_map(
        functools.partial(body, replicas=mesh.shape["dp"]),
        mesh=mesh,
        in_specs=(
            P(("dp", "table"), None),
            P(("dp", "table"), None, None),
            P(("dp", "table"), None, None),
            P(),
            P(),
        ),
        out_specs=P("table", "dp"),
        check_vma=False,
    )
```

```python
import functools

import jax
import jax.numpy as jnp
from jax import lax
from jax.experimental import pallas as pl
from jax.experimental.pallas import tpu as pltpu
from jax.sharding import PartitionSpec as P

ROWS = 128
TOUCH = 32
OWN = 8
CELL_BITS = 12
CODE_BIAS = 128
BLOCK = 128
SIDE = 64
CHUNKS = 8
EARLY = 3


def fill_coef(scale_ref, cells_ref, codes_ref, write, low_ref, high_ref, weight_ref, table_ref):
    pairs, block = cells_ref.shape
    heads = scale_ref.shape[0]
    packed = (cells_ref[...] | ((codes_ref[...] + CODE_BIAS) << CELL_BITS)).T
    stride = table_ref.shape[0] // TOUCH
    tile = (packed >> 7) & (TOUCH - 1)
    upper = (packed >> 6) & 1
    low_ref[...] = (packed & (SIDE - 1)).astype(jnp.float32)
    high_ref[...] = (tile + TOUCH * upper).astype(jnp.float32)
    head = lax.broadcasted_iota(jnp.int32, (1, pairs), 1) // (pairs // heads)
    scale = jnp.zeros((1, pairs), jnp.float32)
    for h in range(heads):
        scale = jnp.where(head == h, scale_ref[h] / 128.0, scale)
    weight_ref[...] = ((packed >> CELL_BITS) - CODE_BIAS).astype(jnp.float32) * scale
    iota = lax.broadcasted_iota(jnp.int32, (SIDE, pairs), 0).astype(jnp.float32).astype(jnp.bfloat16)

    def spread(ref, token):
        row = jnp.broadcast_to(ref[pl.ds(token, 1), :], (16, pairs)).astype(jnp.bfloat16)
        return jnp.concatenate([row] * (SIDE // 16), axis=0)

    for token in range(block):
        low_hot = jnp.where(spread(low_ref, token) == iota, jnp.bfloat16(1), jnp.bfloat16(0))
        high_hot = jnp.where(spread(high_ref, token) == iota, spread(weight_ref, token), jnp.bfloat16(0))
        table = lax.dot_general(
            high_hot, low_hot, (((1,), (1,)), ((), ())), preferred_element_type=jnp.float32
        )
        table = jnp.concatenate([table[:TOUCH], table[TOUCH:]], axis=1)
        table_ref[pl.ds(token, TOUCH, stride=stride), :] = table
    for j in range(TOUCH):
        write(j, table_ref[pl.ds(j * stride, block), :].astype(jnp.bfloat16))


def put_products(flip, coef, out_refs):
    product = jnp.dot(flip, coef, preferred_element_type=jnp.float32)
    for n, out_ref in enumerate(out_refs):
        width = out_ref.shape[2]
        for c in range(out_ref.shape[1]):
            part = product[n * width : (n + 1) * width, c * ROWS : (c + 1) * ROWS]
            out_ref[0, c] = part.astype(jnp.bfloat16)


def first_kernel(place_ref, scale_ref, cells_ref, codes_ref, *refs, groups):
    replicas = (len(refs) - 9) // 2
    grad_refs, (coef_hbm, flip_hbm), out_refs = refs[:replicas], refs[replicas : replicas + 2], refs[replicas + 2 : -7]
    low_ref, high_ref, weight_ref, table_ref, coef_ref, flip_ref, semaphores = refs[-7:]
    step = pl.program_id(0)
    block = cells_ref.shape[1]
    width = grad_refs[0].shape[1]
    blocks = coef_ref.shape[0] // block
    span = coef_ref.shape[1] // groups

    saves = [
        pltpu.make_async_copy(coef_ref, coef_hbm, semaphores.at[0]),
        pltpu.make_async_copy(flip_ref, flip_hbm, semaphores.at[1]),
    ]

    @pl.when(step < blocks)
    def _():
        rows = pl.ds(pl.multiple_of(step * block, block), block)

        def write(j, part):
            coef_ref[rows, j * ROWS : (j + 1) * ROWS] = part

        for n in range(replicas):
            flip_ref[n * width : (n + 1) * width, rows] = grad_refs[n][...].T
        fill_coef(scale_ref, cells_ref, codes_ref, write, low_ref, high_ref, weight_ref, table_ref)

    @pl.when(step >= blocks)
    def _():
        @pl.when(step == blocks)
        def _():
            for copy in saves:
                copy.start()

        owner = place_ref[1] ^ (groups - 1 - (step - blocks))
        coef = coef_ref[:, pl.ds(pl.multiple_of(owner * span, span), span)]
        put_products(flip_ref[...], coef, out_refs)

    @pl.when(step == pl.num_programs(0) - 1)
    def _():
        for copy in saves:
            copy.wait()


def first_products(place, head_scale, cells, codes, grads, replicas, width, capacity, groups, length):
    pairs, tokens = cells.shape
    blocks = tokens // BLOCK
    last = blocks - 1
    spec = pl.BlockSpec((pairs, BLOCK), lambda i, *_: (0, jnp.minimum(i, last)))
    outs = [jax.ShapeDtypeStruct((length, capacity, width, ROWS), jnp.bfloat16) for _ in range(replicas)]
    cells_all = TOUCH * ROWS
    return pl.pallas_call(
        functools.partial(first_kernel, groups=groups),
        grid_spec=pltpu.PrefetchScalarGridSpec(
            num_scalar_prefetch=2,
            grid=(blocks + length,),
            in_specs=[spec, spec]
            + [
                pl.BlockSpec((BLOCK, width), lambda i, place, scale, m=m: (jnp.minimum(i, last), place[0] ^ m))
                for m in range(replicas)
            ],
            out_specs=[pl.BlockSpec(memory_space=pl.ANY), pl.BlockSpec(memory_space=pl.ANY)]
            + [
                pl.BlockSpec((1, capacity, width, ROWS), lambda i, *_: (jnp.maximum(i - blocks, 0), 0, 0, 0))
                for _ in outs
            ],
            scratch_shapes=[
                pltpu.VMEM((BLOCK, pairs), jnp.float32),
                pltpu.VMEM((BLOCK, pairs), jnp.float32),
                pltpu.VMEM((BLOCK, pairs), jnp.float32),
                pltpu.VMEM((TOUCH * (BLOCK + 8), ROWS), jnp.float32),
                pltpu.VMEM((tokens, cells_all), jnp.bfloat16),
                pltpu.VMEM((replicas * width, tokens), jnp.bfloat16),
                pltpu.SemaphoreType.DMA((2,)),
            ],
        ),
        out_shape=[
            jax.ShapeDtypeStruct((tokens, cells_all), jnp.bfloat16),
            jax.ShapeDtypeStruct((replicas * width, tokens), jnp.bfloat16),
        ]
        + outs,
        cost_estimate=pl.CostEstimate(
            flops=2 * tokens * pairs * cells_all * 4, transcendentals=0, bytes_accessed=tokens * cells_all * 4
        ),
        name="first_products",
    )(place, head_scale, cells, codes, *([grads] * replicas))


def rest_kernel(place_ref, coef_ref, flip_ref, after_ref, *out_refs):
    put_products(flip_ref[...], coef_ref[...], out_refs)


def rest_products(place, coef, flip, after, replicas, width, capacity, groups, first):
    tokens = coef.shape[0]
    length = groups - first
    return pl.pallas_call(
        rest_kernel,
        grid_spec=pltpu.PrefetchScalarGridSpec(
            num_scalar_prefetch=1,
            grid=(length,),
            in_specs=[
                pl.BlockSpec((tokens, capacity * ROWS), lambda i, place: (0, place[1] ^ (groups - 1 - first - i))),
                pl.BlockSpec(flip.shape, lambda i, place: (0, 0)),
                pl.BlockSpec(memory_space=pl.ANY),
            ],
            out_specs=[
                pl.BlockSpec((1, capacity, width, ROWS), lambda i, place: (i, 0, 0, 0)) for _ in range(replicas)
            ],
        ),
        out_shape=[
            jax.ShapeDtypeStruct((length, capacity, width, ROWS), jnp.bfloat16) for _ in range(replicas)
        ],
        cost_estimate=pl.CostEstimate(
            flops=2 * tokens * length * capacity * ROWS * width * replicas,
            transcendentals=0,
            bytes_accessed=2 * length * capacity * ROWS * (tokens + replicas * width) + 2 * replicas * width * tokens,
        ),
        name="rest_products",
    )(place, coef, flip, after)


def add_kernel(*refs):
    total = refs[0][...].astype(jnp.float32)
    for ref in refs[1:-1]:
        total = total + ref[...].astype(jnp.float32)
    refs[-1][...] = total.astype(jnp.bfloat16)


def add_blocks(terms, size):
    shape = (size,) + terms[0][0].shape[1:]
    return pl.pallas_call(
        add_kernel,
        grid=(1,),
        in_specs=[pl.BlockSpec(shape, lambda i, n=n: (n, 0, 0, 0)) for _, n in terms],
        out_specs=pl.BlockSpec(shape, lambda i: (0, 0, 0, 0)),
        out_shape=jax.ShapeDtypeStruct(shape, jnp.bfloat16),
        name="add_blocks",
    )(*[array for array, _ in terms])


def gather_kernel(place_ref, slot_ref, *refs):
    groups = (len(refs) - 3) // 2
    part_refs, out_ref = refs[:groups], refs[groups]
    buffer_refs, sum_ref, semaphores = refs[groups + 1 : -2], refs[-2], refs[-1]
    capacity = part_refs[0].shape[0]
    owner = place_ref[1]
    copies = [
        pltpu.make_async_copy(part, buffer, semaphores.at[n])
        for n, (part, buffer) in enumerate(zip(part_refs, buffer_refs))
    ]
    for copy in copies:
        copy.start()
    sum_ref[...] = jnp.zeros(sum_ref.shape, jnp.float32)
    for n in range(groups):
        copies[n].wait()
        for c in range(capacity):
            slot = slot_ref[((owner ^ n) * groups + owner) * capacity + c]
            sum_ref[slot] += buffer_refs[n][c].astype(jnp.float32)
    for k in range(OWN):
        out_ref[pl.ds(k * ROWS, ROWS), :] = sum_ref[k].T.astype(jnp.bfloat16)


def gather_tiles(place, slots, parts):
    capacity, width = parts[0].shape[:2]
    return pl.pallas_call(
        gather_kernel,
        grid_spec=pltpu.PrefetchScalarGridSpec(
            num_scalar_prefetch=2,
            grid=(1,),
            in_specs=[pl.BlockSpec(memory_space=pl.ANY) for _ in parts],
            out_specs=pl.BlockSpec((OWN * ROWS, width), lambda i, place, slots: (0, 0)),
            scratch_shapes=[pltpu.VMEM((capacity, width, ROWS), jnp.bfloat16) for _ in parts]
            + [pltpu.VMEM((OWN, width, ROWS), jnp.float32), pltpu.SemaphoreType.DMA((len(parts),))],
        ),
        out_shape=jax.ShapeDtypeStruct((OWN * ROWS, width), jnp.bfloat16),
        name="gather_tiles",
    )(place, slots, *parts)


def body(out_grad, pair_cells, weight_codes, head_scale, touch_slots, *, replicas):
    tokens, value = out_grad.shape
    width = value // replicas
    groups = touch_slots.shape[0]
    capacity = touch_slots.shape[2]
    pairs = pair_cells.shape[1] * pair_cells.shape[2]
    place = jnp.stack([lax.axis_index("dp"), lax.axis_index("table")]).astype(jnp.int32)
    by_pair = lambda array: array.transpose(1, 2, 0).reshape(pairs, tokens)

    def swap(array, axis, bit):
        return lax.ppermute(array, axis, [(i, i ^ bit) for i in range(lax.axis_size(axis))])

    chunks = min(CHUNKS, groups)
    size = groups // chunks
    early = max(1, EARLY * chunks // CHUNKS) * size
    pieces = [{m: [] for m in range(0, replicas, 2)} for _ in range(chunks)]

    def take(outs, first):
        order = sorted(range(replicas), reverse=True)
        for m in order:
            array = swap(outs[m], "dp", 1) if m & 1 else outs[m]
            for n in range(array.shape[0] // size):
                pieces[first // size + n][m & ~1].append((array, n))

    def send_far(chunk):
        piece = pieces[chunk]
        bit = 2
        while bit < replicas:
            for m in sorted(piece, reverse=True):
                if m & bit:
                    piece[m ^ bit].append((swap(add_blocks(piece.pop(m), size), "dp", bit), 0))
            bit *= 2

    coef, flip, *outs = first_products(
        place, head_scale, by_pair(pair_cells), by_pair(weight_codes), out_grad, replicas, width, capacity, groups, early
    )
    take(outs, 0)
    for chunk in range(early // size):
        send_far(chunk)
    outs = rest_products(place, coef, flip, outs[0], replicas, width, capacity, groups, early)
    take(outs, early)
    for chunk in range(early // size, chunks):
        send_far(chunk)
    parts = {}
    for chunk, piece in enumerate(pieces):
        mine = add_blocks(piece[0], size)
        for i in range(size):
            distance = groups - 1 - chunk * size - i
            part = mine.reshape(mine.shape[1:]) if size == 1 else mine[i]
            parts[distance] = swap(part, "table", distance) if distance else part
    return gather_tiles(place, touch_slots.reshape(-1), [parts[n] for n in range(groups)])


def solution(mesh):
    return jax.shard_map(
        functools.partial(body, replicas=mesh.shape["dp"]),
        mesh=mesh,
        in_specs=(
            P(("dp", "table"), None),
            P(("dp", "table"), None, None),
            P(("dp", "table"), None, None),
            P(),
            P(),
        ),
        out_specs=P("table", "dp"),
        check_vma=False,
    )
```

```python
import functools

import jax
import jax.numpy as jnp
from jax import lax
from jax.experimental import pallas as pl
from jax.experimental.pallas import tpu as pltpu
from jax.sharding import PartitionSpec as P

ROWS = 128
TOUCH = 32
OWN = 8
CELL_BITS = 12
CODE_BIAS = 128
BLOCK = 128
SIDE = 64
CHUNKS = 8
EARLY = 3


def fill_coef(scale_ref, cells_ref, codes_ref, write, low_ref, high_ref, weight_ref, table_ref):
    pairs, block = cells_ref.shape
    heads = scale_ref.shape[0]
    packed = (cells_ref[...] | ((codes_ref[...] + CODE_BIAS) << CELL_BITS)).T
    stride = table_ref.shape[0] // TOUCH
    tile = (packed >> 7) & (TOUCH - 1)
    upper = (packed >> 6) & 1
    low_ref[...] = (packed & (SIDE - 1)).astype(jnp.float32)
    high_ref[...] = (tile + TOUCH * upper).astype(jnp.float32)
    head = lax.broadcasted_iota(jnp.int32, (1, pairs), 1) // (pairs // heads)
    scale = jnp.zeros((1, pairs), jnp.float32)
    for h in range(heads):
        scale = jnp.where(head == h, scale_ref[h] / 128.0, scale)
    weight_ref[...] = ((packed >> CELL_BITS) - CODE_BIAS).astype(jnp.float32) * scale
    iota = lax.broadcasted_iota(jnp.int32, (SIDE, pairs), 0).astype(jnp.float32).astype(jnp.bfloat16)

    def spread(ref, token):
        row = jnp.broadcast_to(ref[pl.ds(token, 1), :], (16, pairs)).astype(jnp.bfloat16)
        return jnp.concatenate([row] * (SIDE // 16), axis=0)

    for token in range(block):
        low_hot = jnp.where(spread(low_ref, token) == iota, jnp.bfloat16(1), jnp.bfloat16(0))
        high_hot = jnp.where(spread(high_ref, token) == iota, spread(weight_ref, token), jnp.bfloat16(0))
        table = lax.dot_general(
            high_hot, low_hot, (((1,), (1,)), ((), ())), preferred_element_type=jnp.float32
        )
        table = jnp.concatenate([table[:TOUCH], table[TOUCH:]], axis=1)
        table_ref[pl.ds(token, TOUCH, stride=stride), :] = table
    for j in range(TOUCH):
        write(j, table_ref[pl.ds(j * stride, block), :].astype(jnp.bfloat16))


def put_products(flip, coef, out_refs):
    product = jnp.dot(flip, coef, preferred_element_type=jnp.float32)
    for n, out_ref in enumerate(out_refs):
        width = out_ref.shape[2]
        for c in range(out_ref.shape[1]):
            part = product[n * width : (n + 1) * width, c * ROWS : (c + 1) * ROWS]
            out_ref[0, c] = part.astype(jnp.bfloat16)


def first_kernel(place_ref, scale_ref, cells_ref, codes_ref, *refs, groups):
    replicas = (len(refs) - 9) // 2
    grad_refs, (coef_hbm, flip_hbm), out_refs = refs[:replicas], refs[replicas : replicas + 2], refs[replicas + 2 : -7]
    low_ref, high_ref, weight_ref, table_ref, coef_ref, flip_ref, semaphores = refs[-7:]
    step = pl.program_id(0)
    block = cells_ref.shape[1]
    width = grad_refs[0].shape[1]
    blocks = coef_ref.shape[0] // block
    span = coef_ref.shape[1] // groups

    saves = [
        pltpu.make_async_copy(coef_ref, coef_hbm, semaphores.at[0]),
        pltpu.make_async_copy(flip_ref, flip_hbm, semaphores.at[1]),
    ]

    @pl.when(step < blocks)
    def _():
        rows = pl.ds(pl.multiple_of(step * block, block), block)

        def write(j, part):
            coef_ref[rows, j * ROWS : (j + 1) * ROWS] = part

        for n in range(replicas):
            flip_ref[n * width : (n + 1) * width, rows] = grad_refs[n][...].T
        fill_coef(scale_ref, cells_ref, codes_ref, write, low_ref, high_ref, weight_ref, table_ref)

    @pl.when(step >= blocks)
    def _():
        @pl.when(step == blocks)
        def _():
            for copy in saves:
                copy.start()

        owner = place_ref[1] ^ (groups - 1 - (step - blocks))
        coef = coef_ref[:, pl.ds(pl.multiple_of(owner * span, span), span)]
        put_products(flip_ref[...], coef, out_refs)

    @pl.when(step == pl.num_programs(0) - 1)
    def _():
        for copy in saves:
            copy.wait()


def first_products(place, head_scale, cells, codes, grads, replicas, width, capacity, groups, length):
    pairs, tokens = cells.shape
    blocks = tokens // BLOCK
    last = blocks - 1
    spec = pl.BlockSpec((pairs, BLOCK), lambda i, *_: (0, jnp.minimum(i, last)))
    outs = [jax.ShapeDtypeStruct((length, capacity, width, ROWS), jnp.bfloat16) for _ in range(replicas)]
    cells_all = TOUCH * ROWS
    return pl.pallas_call(
        functools.partial(first_kernel, groups=groups),
        grid_spec=pltpu.PrefetchScalarGridSpec(
            num_scalar_prefetch=2,
            grid=(blocks + length,),
            in_specs=[spec, spec]
            + [
                pl.BlockSpec((BLOCK, width), lambda i, place, scale, m=m: (jnp.minimum(i, last), place[0] ^ m))
                for m in range(replicas)
            ],
            out_specs=[pl.BlockSpec(memory_space=pl.ANY), pl.BlockSpec(memory_space=pl.ANY)]
            + [
                pl.BlockSpec((1, capacity, width, ROWS), lambda i, *_: (jnp.maximum(i - blocks, 0), 0, 0, 0))
                for _ in outs
            ],
            scratch_shapes=[
                pltpu.VMEM((BLOCK, pairs), jnp.float32),
                pltpu.VMEM((BLOCK, pairs), jnp.float32),
                pltpu.VMEM((BLOCK, pairs), jnp.float32),
                pltpu.VMEM((TOUCH * (BLOCK + 8), ROWS), jnp.float32),
                pltpu.VMEM((tokens, cells_all), jnp.bfloat16),
                pltpu.VMEM((replicas * width, tokens), jnp.bfloat16),
                pltpu.SemaphoreType.DMA((2,)),
            ],
        ),
        out_shape=[
            jax.ShapeDtypeStruct((tokens, cells_all), jnp.bfloat16),
            jax.ShapeDtypeStruct((replicas * width, tokens), jnp.bfloat16),
        ]
        + outs,
        cost_estimate=pl.CostEstimate(
            flops=2 * tokens * pairs * cells_all * 4, transcendentals=0, bytes_accessed=tokens * cells_all * 4
        ),
        compiler_params=pltpu.CompilerParams(vmem_limit_bytes=30 << 20),
        name="first_products",
    )(place, head_scale, cells, codes, *([grads] * replicas))


def rest_kernel(place_ref, coef_ref, flip_ref, after_ref, *out_refs):
    put_products(flip_ref[...], coef_ref[...], out_refs)


def rest_products(place, coef, flip, after, replicas, width, capacity, groups, first):
    tokens = coef.shape[0]
    length = groups - first
    return pl.pallas_call(
        rest_kernel,
        grid_spec=pltpu.PrefetchScalarGridSpec(
            num_scalar_prefetch=1,
            grid=(length,),
            in_specs=[
                pl.BlockSpec((tokens, capacity * ROWS), lambda i, place: (0, place[1] ^ (groups - 1 - first - i))),
                pl.BlockSpec(flip.shape, lambda i, place: (0, 0)),
                pl.BlockSpec(memory_space=pl.ANY),
            ],
            out_specs=[
                pl.BlockSpec((1, capacity, width, ROWS), lambda i, place: (i, 0, 0, 0)) for _ in range(replicas)
            ],
        ),
        out_shape=[
            jax.ShapeDtypeStruct((length, capacity, width, ROWS), jnp.bfloat16) for _ in range(replicas)
        ],
        cost_estimate=pl.CostEstimate(
            flops=2 * tokens * length * capacity * ROWS * width * replicas,
            transcendentals=0,
            bytes_accessed=2 * length * capacity * ROWS * (tokens + replicas * width) + 2 * replicas * width * tokens,
        ),
        compiler_params=pltpu.CompilerParams(vmem_limit_bytes=24 << 20),
        name="rest_products",
    )(place, coef, flip, after)


def add_kernel(*refs, plan):
    count = len(refs) - len(plan)
    for out_ref, terms in zip(refs[count:], plan):
        size = out_ref.shape[0]
        total = 0.0
        for n, at in terms:
            total = total + refs[n][at * size : (at + 1) * size].astype(jnp.float32)
        out_ref[...] = total.astype(jnp.bfloat16)


def add_blocks(sums, size):
    arrays = []
    plan = []
    for terms in sums:
        row = []
        for array, at in terms:
            known = [n for n, other in enumerate(arrays) if other is array]
            if not known:
                known = [len(arrays)]
                arrays.append(array)
            row.append((known[0], at))
        plan.append(tuple(row))
    shape = (size,) + arrays[0].shape[1:]
    spec = pl.BlockSpec(memory_space=pltpu.VMEM)
    return pl.pallas_call(
        functools.partial(add_kernel, plan=tuple(plan)),
        in_specs=[spec for _ in arrays],
        out_specs=[spec for _ in plan],
        out_shape=[pltpu.VMEM(shape, jnp.bfloat16) for _ in plan],
        compiler_params=pltpu.CompilerParams(vmem_limit_bytes=4 << 20),
        name="add_blocks",
    )(*[pltpu.with_memory_space_constraint(array, pltpu.VMEM) for array in arrays])


def gather_kernel(place_ref, slot_ref, *refs):
    part_refs, out_ref, sum_ref = refs[:-2], refs[-2], refs[-1]
    groups = len(part_refs)
    capacity = part_refs[0].shape[1]
    owner = place_ref[1]
    sum_ref[...] = jnp.zeros(sum_ref.shape, jnp.float32)
    for n, part_ref in enumerate(part_refs):
        for c in range(capacity):
            slot = slot_ref[((owner ^ n) * groups + owner) * capacity + c]
            sum_ref[slot] += part_ref[0, c].astype(jnp.float32)
    for k in range(OWN):
        out_ref[pl.ds(k * ROWS, ROWS), :] = sum_ref[k].T.astype(jnp.bfloat16)


def gather_tiles(place, slots, parts):
    width = parts[0].shape[2]
    scalars = pl.BlockSpec(memory_space=pltpu.SMEM)
    spec = pl.BlockSpec(memory_space=pltpu.VMEM)
    return pl.pallas_call(
        gather_kernel,
        in_specs=[scalars, scalars] + [spec for _ in parts],
        out_specs=spec,
        scratch_shapes=[pltpu.VMEM((OWN, width, ROWS), jnp.float32)],
        out_shape=jax.ShapeDtypeStruct((OWN * ROWS, width), jnp.bfloat16),
        compiler_params=pltpu.CompilerParams(vmem_limit_bytes=6 << 20),
        name="gather_tiles",
    )(place, slots, *[pltpu.with_memory_space_constraint(part, pltpu.VMEM) for part in parts])


def body(out_grad, pair_cells, weight_codes, head_scale, touch_slots, *, replicas):
    tokens, value = out_grad.shape
    width = value // replicas
    groups = touch_slots.shape[0]
    capacity = touch_slots.shape[2]
    pairs = pair_cells.shape[1] * pair_cells.shape[2]
    place = jnp.stack([lax.axis_index("dp"), lax.axis_index("table")]).astype(jnp.int32)
    by_pair = lambda array: array.transpose(1, 2, 0).reshape(pairs, tokens)

    def swap(array, axis, bit):
        return lax.ppermute(array, axis, [(i, i ^ bit) for i in range(lax.axis_size(axis))])

    chunks = min(CHUNKS, groups)
    size = groups // chunks
    early = max(1, EARLY * chunks // CHUNKS) * size
    pieces = [{m: [] for m in range(0, replicas, 2)} for _ in range(chunks)]

    def take(outs, first):
        order = sorted(range(replicas), reverse=True)
        for m in order:
            array = swap(outs[m], "dp", 1) if m & 1 else outs[m]
            for n in range(array.shape[0] // size):
                pieces[first // size + n][m & ~1].append((array, n))

    def send_far(first, stop):
        some = pieces[first:stop]
        bit = 2
        sent = None
        while bit < replicas:
            masks = [m for m in sorted(some[0], reverse=True) if m & bit]
            sums = iter(add_blocks([piece.pop(m) for piece in some for m in masks], size))
            for piece in some:
                for m in masks:
                    total = next(sums)
                    sent = total if sent is None else sent
                    piece[m ^ bit].append((swap(total, "dp", bit), 0))
            bit *= 2
        return sent

    coef, flip, *outs = first_products(
        place, head_scale, by_pair(pair_cells), by_pair(weight_codes), out_grad, replicas, width, capacity, groups, early
    )
    take(outs, 0)
    sent = send_far(0, early // size)
    outs = rest_products(
        place, coef, flip, outs[0] if sent is None else sent, replicas, width, capacity, groups, early
    )
    take(outs, early)
    send_far(early // size, chunks)
    parts = {}
    for chunk, piece in enumerate(pieces):
        (mine,) = add_blocks([piece[0]], size)
        for i in range(size):
            distance = groups - 1 - chunk * size - i
            part = mine if size == 1 else mine[i : i + 1]
            parts[distance] = swap(part, "table", distance) if distance else part
    return gather_tiles(place, touch_slots.reshape(-1), [parts[n] for n in range(groups)])


def solution(mesh):
    return jax.shard_map(
        functools.partial(body, replicas=mesh.shape["dp"]),
        mesh=mesh,
        in_specs=(
            P(("dp", "table"), None),
            P(("dp", "table"), None, None),
            P(("dp", "table"), None, None),
            P(),
            P(),
        ),
        out_specs=P("table", "dp"),
        check_vma=False,
    )
```

```python
import functools

import jax
import jax.numpy as jnp
from jax import lax
from jax.experimental import pallas as pl
from jax.experimental.pallas import tpu as pltpu
from jax.sharding import PartitionSpec as P


ROWS = 128
TOUCH = 32
OWN = 8
CELL_BITS = 12
CODE_BIAS = 128
BLOCK = 128
SIDE = 64
CHUNKS = 8
EARLY = 3


def fill_coef(scale_ref, cells_ref, codes_ref, write, low_ref, high_ref, weight_ref, table_ref):
    pairs, block = cells_ref.shape
    heads = scale_ref.shape[0]
    packed = (cells_ref[...] | ((codes_ref[...] + CODE_BIAS) << CELL_BITS)).T
    stride = table_ref.shape[0] // TOUCH
    tile = (packed >> 7) & (TOUCH - 1)
    upper = (packed >> 6) & 1
    low_ref[...] = (packed & (SIDE - 1)).astype(jnp.float32)
    high_ref[...] = (tile + TOUCH * upper).astype(jnp.float32)
    head = lax.broadcasted_iota(jnp.int32, (1, pairs), 1) // (pairs // heads)
    scale = jnp.zeros((1, pairs), jnp.float32)
    for h in range(heads):
        scale = jnp.where(head == h, scale_ref[h] / 128.0, scale)
    weight_ref[...] = ((packed >> CELL_BITS) - CODE_BIAS).astype(jnp.float32) * scale
    iota = lax.broadcasted_iota(jnp.int32, (SIDE, pairs), 0).astype(jnp.float32).astype(jnp.bfloat16)

    def spread(ref, token):
        row = jnp.broadcast_to(ref[pl.ds(token, 1), :], (16, pairs)).astype(jnp.bfloat16)
        return jnp.concatenate([row] * (SIDE // 16), axis=0)

    for token in range(block):
        low_hot = jnp.where(spread(low_ref, token) == iota, jnp.bfloat16(1), jnp.bfloat16(0))
        high_hot = jnp.where(spread(high_ref, token) == iota, spread(weight_ref, token), jnp.bfloat16(0))
        table = lax.dot_general(
            high_hot, low_hot, (((1,), (1,)), ((), ())), preferred_element_type=jnp.float32
        )
        table = jnp.concatenate([table[:TOUCH], table[TOUCH:]], axis=1)
        table_ref[pl.ds(token, TOUCH, stride=stride), :] = table
    for j in range(TOUCH):
        write(j, table_ref[pl.ds(j * stride, block), :].astype(jnp.bfloat16))


def distance_at(position, groups):
    half = groups // 2
    if isinstance(position, int):
        return half + position if position < half else groups - 1 - position
    return jnp.where(position < half, half + position, groups - 1 - position)


def put_products(flip, coef, out_refs):
    product = jnp.dot(flip, coef, preferred_element_type=jnp.float32)
    for n, out_ref in enumerate(out_refs):
        width = out_ref.shape[2]
        for c in range(out_ref.shape[1]):
            part = product[n * width : (n + 1) * width, c * ROWS : (c + 1) * ROWS]
            out_ref[0, c] = part.astype(jnp.bfloat16)


def first_kernel(place_ref, scale_ref, cells_ref, codes_ref, *refs, groups):
    replicas = (len(refs) - 9) // 2
    grad_refs, (coef_hbm, flip_hbm), out_refs = refs[:replicas], refs[replicas : replicas + 2], refs[replicas + 2 : -7]
    low_ref, high_ref, weight_ref, table_ref, coef_ref, flip_ref, semaphores = refs[-7:]
    step = pl.program_id(0)
    block = cells_ref.shape[1]
    width = grad_refs[0].shape[1]
    blocks = coef_ref.shape[0] // block
    span = coef_ref.shape[1] // groups

    saves = [
        pltpu.make_async_copy(coef_ref, coef_hbm, semaphores.at[0]),
        pltpu.make_async_copy(flip_ref, flip_hbm, semaphores.at[1]),
    ]

    @pl.when(step < blocks)
    def _():
        rows = pl.ds(pl.multiple_of(step * block, block), block)

        def write(j, part):
            coef_ref[rows, j * ROWS : (j + 1) * ROWS] = part

        for n in range(replicas):
            flip_ref[n * width : (n + 1) * width, rows] = grad_refs[n][...].T
        fill_coef(scale_ref, cells_ref, codes_ref, write, low_ref, high_ref, weight_ref, table_ref)

    @pl.when(step >= blocks)
    def _():
        @pl.when(step == blocks)
        def _():
            for copy in saves:
                copy.start()

        owner = place_ref[1] ^ distance_at(step - blocks, groups)
        coef = coef_ref[:, pl.ds(pl.multiple_of(owner * span, span), span)]
        put_products(flip_ref[...], coef, out_refs)

    @pl.when(step == pl.num_programs(0) - 1)
    def _():
        for copy in saves:
            copy.wait()


def first_products(place, head_scale, cells, codes, grads, replicas, width, capacity, groups, length):
    pairs, tokens = cells.shape
    blocks = tokens // BLOCK
    last = blocks - 1
    spec = pl.BlockSpec((pairs, BLOCK), lambda i, *_: (0, jnp.minimum(i, last)))
    outs = [jax.ShapeDtypeStruct((length, capacity, width, ROWS), jnp.bfloat16) for _ in range(replicas)]
    cells_all = TOUCH * ROWS
    return pl.pallas_call(
        functools.partial(first_kernel, groups=groups),
        grid_spec=pltpu.PrefetchScalarGridSpec(
            num_scalar_prefetch=2,
            grid=(blocks + length,),
            in_specs=[spec, spec]
            + [
                pl.BlockSpec((BLOCK, width), lambda i, place, scale, m=m: (jnp.minimum(i, last), place[0] ^ m))
                for m in range(replicas)
            ],
            out_specs=[pl.BlockSpec(memory_space=pl.ANY), pl.BlockSpec(memory_space=pl.ANY)]
            + [
                pl.BlockSpec((1, capacity, width, ROWS), lambda i, *_: (jnp.maximum(i - blocks, 0), 0, 0, 0))
                for _ in outs
            ],
            scratch_shapes=[
                pltpu.VMEM((BLOCK, pairs), jnp.float32),
                pltpu.VMEM((BLOCK, pairs), jnp.float32),
                pltpu.VMEM((BLOCK, pairs), jnp.float32),
                pltpu.VMEM((TOUCH * (BLOCK + 8), ROWS), jnp.float32),
                pltpu.VMEM((tokens, cells_all), jnp.bfloat16),
                pltpu.VMEM((replicas * width, tokens), jnp.bfloat16),
                pltpu.SemaphoreType.DMA((2,)),
            ],
        ),
        out_shape=[
            jax.ShapeDtypeStruct((tokens, cells_all), jnp.bfloat16),
            jax.ShapeDtypeStruct((replicas * width, tokens), jnp.bfloat16),
        ]
        + outs,
        cost_estimate=pl.CostEstimate(
            flops=2 * tokens * pairs * cells_all * 4, transcendentals=0, bytes_accessed=tokens * cells_all * 4
        ),
        compiler_params=pltpu.CompilerParams(vmem_limit_bytes=30 << 20),
        name="first_products",
    )(place, head_scale, *[pltpu.with_memory_space_constraint(a, pltpu.HBM) for a in [cells, codes] + [grads] * replicas])


def rest_kernel(place_ref, coef_ref, flip_ref, after_ref, *out_refs):
    put_products(flip_ref[...], coef_ref[...], out_refs)


def rest_products(place, coef, flip, after, replicas, width, capacity, groups, first):
    tokens = coef.shape[0]
    length = groups - first
    return pl.pallas_call(
        rest_kernel,
        grid_spec=pltpu.PrefetchScalarGridSpec(
            num_scalar_prefetch=1,
            grid=(length,),
            in_specs=[
                pl.BlockSpec((tokens, capacity * ROWS), lambda i, place: (0, place[1] ^ distance_at(first + i, groups))),
                pl.BlockSpec(flip.shape, lambda i, place: (0, 0)),
                pl.BlockSpec(memory_space=pl.ANY),
            ],
            out_specs=[
                pl.BlockSpec((1, capacity, width, ROWS), lambda i, place: (i, 0, 0, 0)) for _ in range(replicas)
            ],
        ),
        out_shape=[
            jax.ShapeDtypeStruct((length, capacity, width, ROWS), jnp.bfloat16) for _ in range(replicas)
        ],
        cost_estimate=pl.CostEstimate(
            flops=2 * tokens * length * capacity * ROWS * width * replicas,
            transcendentals=0,
            bytes_accessed=2 * length * capacity * ROWS * (tokens + replicas * width) + 2 * replicas * width * tokens,
        ),
        compiler_params=pltpu.CompilerParams(vmem_limit_bytes=24 << 20),
        name="rest_products",
    )(place, coef, flip, after)


def add_kernel(*refs, plan):
    count = len(refs) - len(plan)
    for out_ref, terms in zip(refs[count:], plan):
        size = out_ref.shape[0]
        total = 0.0
        for n, at in terms:
            total = total + refs[n][at * size : (at + 1) * size].astype(jnp.float32)
        out_ref[...] = total.astype(jnp.bfloat16)


def add_blocks(sums, size):
    arrays = []
    plan = []
    for terms in sums:
        row = []
        for array, at in terms:
            known = [n for n, other in enumerate(arrays) if other is array]
            if not known:
                known = [len(arrays)]
                arrays.append(array)
            row.append((known[0], at))
        plan.append(tuple(row))
    shape = (size,) + arrays[0].shape[1:]
    spec = pl.BlockSpec(memory_space=pltpu.VMEM)
    return pl.pallas_call(
        functools.partial(add_kernel, plan=tuple(plan)),
        in_specs=[spec for _ in arrays],
        out_specs=[spec for _ in plan],
        out_shape=[pltpu.VMEM(shape, jnp.bfloat16) for _ in plan],
        compiler_params=pltpu.CompilerParams(vmem_limit_bytes=4 << 20),
        name="add_blocks",
    )(*[pltpu.with_memory_space_constraint(array, pltpu.VMEM) for array in arrays])


def gather_kernel(place_ref, slot_ref, *refs):
    part_refs, out_ref, sum_ref = refs[:-2], refs[-2], refs[-1]
    groups = len(part_refs)
    capacity = part_refs[0].shape[1]
    owner = place_ref[1]
    sum_ref[...] = jnp.zeros(sum_ref.shape, jnp.float32)
    for n, part_ref in enumerate(part_refs):
        for c in range(capacity):
            slot = slot_ref[((owner ^ n) * groups + owner) * capacity + c]
            sum_ref[slot] += part_ref[0, c].astype(jnp.float32)
    for k in range(OWN):
        out_ref[pl.ds(k * ROWS, ROWS), :] = sum_ref[k].T.astype(jnp.bfloat16)


def gather_tiles(place, slots, parts):
    width = parts[0].shape[2]
    scalars = pl.BlockSpec(memory_space=pltpu.SMEM)
    spec = pl.BlockSpec(memory_space=pltpu.VMEM)
    return pl.pallas_call(
        gather_kernel,
        in_specs=[scalars, scalars] + [spec for _ in parts],
        out_specs=spec,
        scratch_shapes=[pltpu.VMEM((OWN, width, ROWS), jnp.float32)],
        out_shape=jax.ShapeDtypeStruct((OWN * ROWS, width), jnp.bfloat16),
        compiler_params=pltpu.CompilerParams(vmem_limit_bytes=6 << 20),
        name="gather_tiles",
    )(place, slots, *[pltpu.with_memory_space_constraint(part, pltpu.VMEM) for part in parts])


def body(out_grad, pair_cells, weight_codes, head_scale, touch_slots, *, replicas):
    tokens, value = out_grad.shape
    width = value // replicas
    groups = touch_slots.shape[0]
    capacity = touch_slots.shape[2]
    pairs = pair_cells.shape[1] * pair_cells.shape[2]
    place = jnp.stack([lax.axis_index("dp"), lax.axis_index("table")]).astype(jnp.int32)
    by_pair = lambda array: array.transpose(1, 2, 0).reshape(pairs, tokens)

    def swap(array, axis, bit):
        return lax.ppermute(array, axis, [(i, i ^ bit) for i in range(lax.axis_size(axis))])

    chunks = min(CHUNKS, groups)
    size = groups // chunks
    early = max(1, EARLY * chunks // CHUNKS) * size
    pieces = [{m: [] for m in range(0, replicas, 2)} for _ in range(chunks)]

    def take(outs, first):
        order = sorted(range(replicas), reverse=True)
        for m in order:
            array = swap(outs[m], "dp", 1) if m & 1 else outs[m]
            for n in range(array.shape[0] // size):
                pieces[first // size + n][m & ~1].append((array, n))

    def send_far(first, stop):
        some = pieces[first:stop]
        bit = 2
        sent = None
        while bit < replicas:
            masks = [m for m in sorted(some[0], reverse=True) if m & bit]
            sums = iter(add_blocks([piece.pop(m) for piece in some for m in masks], size))
            for piece in some:
                for m in masks:
                    total = next(sums)
                    sent = total if sent is None else sent
                    piece[m ^ bit].append((swap(total, "dp", bit), 0))
            bit *= 2
        return sent

    coef, flip, *outs = first_products(
        place, head_scale, by_pair(pair_cells), by_pair(weight_codes), out_grad, replicas, width, capacity, groups, early
    )
    take(outs, 0)
    sent = send_far(0, early // size)
    outs = rest_products(place, coef, flip, outs[0] if sent is None else sent, replicas, width, capacity, groups, early)
    take(outs, early)
    send_far(early // size, chunks)
    parts = {}
    for chunk, piece in enumerate(pieces):
        (mine,) = add_blocks([piece[0]], size)
        for i in range(size):
            distance = distance_at(chunk * size + i, groups)
            part = mine if size == 1 else mine[i : i + 1]
            parts[distance] = swap(part, "table", distance) if distance else part
    return gather_tiles(place, touch_slots.reshape(-1), [parts[n] for n in range(groups)])


def solution(mesh):
    return jax.shard_map(
        functools.partial(body, replicas=mesh.shape["dp"]),
        mesh=mesh,
        in_specs=(
            P(("dp", "table"), None),
            P(("dp", "table"), None, None),
            P(("dp", "table"), None, None),
            P(),
            P(),
        ),
        out_specs=P("table", "dp"),
        check_vma=False,
    )
```

```python
import functools

import jax
import jax.numpy as jnp
from jax import lax
from jax.experimental import pallas as pl
from jax.experimental.pallas import tpu as pltpu
from jax.sharding import PartitionSpec as P


ROWS = 128
TOUCH = 32
OWN = 8
CELL_BITS = 12
CODE_BIAS = 128
BLOCK = 128
SIDE = 64
CHUNKS = 8
EDGES = (0, 2, 4, 8)


def fill_coef(scale_ref, cells_ref, codes_ref, write, low_ref, high_ref, weight_ref, table_ref):
    pairs, block = cells_ref.shape
    heads = scale_ref.shape[0]
    packed = (cells_ref[...] | ((codes_ref[...] + CODE_BIAS) << CELL_BITS)).T
    stride = table_ref.shape[0] // TOUCH
    tile = (packed >> 7) & (TOUCH - 1)
    upper = (packed >> 6) & 1
    low_ref[...] = (packed & (SIDE - 1)).astype(jnp.float32)
    high_ref[...] = (tile + TOUCH * upper).astype(jnp.float32)
    head = lax.broadcasted_iota(jnp.int32, (1, pairs), 1) // (pairs // heads)
    scale = jnp.zeros((1, pairs), jnp.float32)
    for h in range(heads):
        scale = jnp.where(head == h, scale_ref[h] / 128.0, scale)
    weight_ref[...] = ((packed >> CELL_BITS) - CODE_BIAS).astype(jnp.float32) * scale
    iota = lax.broadcasted_iota(jnp.int32, (SIDE, pairs), 0).astype(jnp.float32).astype(jnp.bfloat16)

    def spread(ref, token):
        row = jnp.broadcast_to(ref[pl.ds(token, 1), :], (16, pairs)).astype(jnp.bfloat16)
        return jnp.concatenate([row] * (SIDE // 16), axis=0)

    for token in range(block):
        low_hot = jnp.where(spread(low_ref, token) == iota, jnp.bfloat16(1), jnp.bfloat16(0))
        high_hot = jnp.where(spread(high_ref, token) == iota, spread(weight_ref, token), jnp.bfloat16(0))
        table = lax.dot_general(
            high_hot, low_hot, (((1,), (1,)), ((), ())), preferred_element_type=jnp.float32
        )
        table = jnp.concatenate([table[:TOUCH], table[TOUCH:]], axis=1)
        table_ref[pl.ds(token, TOUCH, stride=stride), :] = table
    for j in range(TOUCH):
        write(j, table_ref[pl.ds(j * stride, block), :].astype(jnp.bfloat16))


def distance_at(position, groups):
    half = groups // 2
    if isinstance(position, int):
        return half + position if position < half else groups - 1 - position
    return jnp.where(position < half, half + position, groups - 1 - position)


def put_products(flip, coef, out_refs):
    product = jnp.dot(flip, coef, preferred_element_type=jnp.float32)
    for n, out_ref in enumerate(out_refs):
        width = out_ref.shape[2]
        for c in range(out_ref.shape[1]):
            part = product[n * width : (n + 1) * width, c * ROWS : (c + 1) * ROWS]
            out_ref[0, c] = part.astype(jnp.bfloat16)


def first_kernel(place_ref, scale_ref, cells_ref, codes_ref, *refs, groups):
    replicas = (len(refs) - 9) // 2
    grad_refs, (coef_hbm, flip_hbm), out_refs = refs[:replicas], refs[replicas : replicas + 2], refs[replicas + 2 : -7]
    low_ref, high_ref, weight_ref, table_ref, coef_ref, flip_ref, semaphores = refs[-7:]
    step = pl.program_id(0)
    block = cells_ref.shape[1]
    width = grad_refs[0].shape[1]
    blocks = coef_ref.shape[0] // block
    span = coef_ref.shape[1] // groups

    saves = [
        pltpu.make_async_copy(coef_ref, coef_hbm, semaphores.at[0]),
        pltpu.make_async_copy(flip_ref, flip_hbm, semaphores.at[1]),
    ]

    @pl.when(step < blocks)
    def _():
        rows = pl.ds(pl.multiple_of(step * block, block), block)

        def write(j, part):
            coef_ref[rows, j * ROWS : (j + 1) * ROWS] = part

        for n in range(replicas):
            flip_ref[n * width : (n + 1) * width, rows] = grad_refs[n][...].T
        fill_coef(scale_ref, cells_ref, codes_ref, write, low_ref, high_ref, weight_ref, table_ref)

    @pl.when(step >= blocks)
    def _():
        @pl.when(step == blocks)
        def _():
            for copy in saves:
                copy.start()

        owner = place_ref[1] ^ distance_at(step - blocks, groups)
        coef = coef_ref[:, pl.ds(pl.multiple_of(owner * span, span), span)]
        put_products(flip_ref[...], coef, out_refs)

    @pl.when(step == pl.num_programs(0) - 1)
    def _():
        for copy in saves:
            copy.wait()


def first_products(place, head_scale, cells, codes, grads, replicas, width, capacity, groups, length):
    pairs, tokens = cells.shape
    blocks = tokens // BLOCK
    last = blocks - 1
    spec = pl.BlockSpec((pairs, BLOCK), lambda i, *_: (0, jnp.minimum(i, last)))
    outs = [jax.ShapeDtypeStruct((length, capacity, width, ROWS), jnp.bfloat16) for _ in range(replicas)]
    cells_all = TOUCH * ROWS
    return pl.pallas_call(
        functools.partial(first_kernel, groups=groups),
        grid_spec=pltpu.PrefetchScalarGridSpec(
            num_scalar_prefetch=2,
            grid=(blocks + length,),
            in_specs=[spec, spec]
            + [
                pl.BlockSpec((BLOCK, width), lambda i, place, scale, m=m: (jnp.minimum(i, last), place[0] ^ m))
                for m in range(replicas)
            ],
            out_specs=[pl.BlockSpec(memory_space=pl.ANY), pl.BlockSpec(memory_space=pl.ANY)]
            + [
                pl.BlockSpec((1, capacity, width, ROWS), lambda i, *_: (jnp.maximum(i - blocks, 0), 0, 0, 0))
                for _ in outs
            ],
            scratch_shapes=[
                pltpu.VMEM((BLOCK, pairs), jnp.float32),
                pltpu.VMEM((BLOCK, pairs), jnp.float32),
                pltpu.VMEM((BLOCK, pairs), jnp.float32),
                pltpu.VMEM((TOUCH * (BLOCK + 8), ROWS), jnp.float32),
                pltpu.VMEM((tokens, cells_all), jnp.bfloat16),
                pltpu.VMEM((replicas * width, tokens), jnp.bfloat16),
                pltpu.SemaphoreType.DMA((2,)),
            ],
        ),
        out_shape=[
            jax.ShapeDtypeStruct((tokens, cells_all), jnp.bfloat16),
            jax.ShapeDtypeStruct((replicas * width, tokens), jnp.bfloat16),
        ]
        + outs,
        cost_estimate=pl.CostEstimate(
            flops=2 * tokens * pairs * cells_all * 4, transcendentals=0, bytes_accessed=tokens * cells_all * 4
        ),
        compiler_params=pltpu.CompilerParams(vmem_limit_bytes=30 << 20),
        name="first_products",
    )(place, head_scale, *[pltpu.with_memory_space_constraint(a, pltpu.HBM) for a in [cells, codes] + [grads] * replicas])


def rest_kernel(place_ref, coef_ref, flip_ref, after_ref, *out_refs):
    put_products(flip_ref[...], coef_ref[...], out_refs)


def rest_products(place, coef, flip, after, replicas, width, capacity, groups, first, stop):
    tokens = coef.shape[0]
    length = stop - first
    return pl.pallas_call(
        rest_kernel,
        grid_spec=pltpu.PrefetchScalarGridSpec(
            num_scalar_prefetch=1,
            grid=(length,),
            in_specs=[
                pl.BlockSpec((tokens, capacity * ROWS), lambda i, place: (0, place[1] ^ distance_at(first + i, groups))),
                pl.BlockSpec(flip.shape, lambda i, place: (0, 0)),
                pl.BlockSpec(memory_space=pl.ANY),
            ],
            out_specs=[
                pl.BlockSpec((1, capacity, width, ROWS), lambda i, place: (i, 0, 0, 0)) for _ in range(replicas)
            ],
        ),
        out_shape=[
            jax.ShapeDtypeStruct((length, capacity, width, ROWS), jnp.bfloat16) for _ in range(replicas)
        ],
        cost_estimate=pl.CostEstimate(
            flops=2 * tokens * length * capacity * ROWS * width * replicas,
            transcendentals=0,
            bytes_accessed=2 * length * capacity * ROWS * (tokens + replicas * width) + 2 * replicas * width * tokens,
        ),
        compiler_params=pltpu.CompilerParams(vmem_limit_bytes=24 << 20),
        name="rest_products",
    )(place, coef, flip, after)


def add_kernel(*refs, plan):
    count = len(refs) - len(plan)
    for out_ref, terms in zip(refs[count:], plan):
        size = out_ref.shape[0]
        total = 0.0
        for n, at in terms:
            total = total + refs[n][at * size : (at + 1) * size].astype(jnp.float32)
        out_ref[...] = total.astype(jnp.bfloat16)


def add_blocks(sums, size):
    arrays = []
    plan = []
    for terms in sums:
        row = []
        for array, at in terms:
            known = [n for n, other in enumerate(arrays) if other is array]
            if not known:
                known = [len(arrays)]
                arrays.append(array)
            row.append((known[0], at))
        plan.append(tuple(row))
    shape = (size,) + arrays[0].shape[1:]
    spec = pl.BlockSpec(memory_space=pltpu.VMEM)
    return pl.pallas_call(
        functools.partial(add_kernel, plan=tuple(plan)),
        in_specs=[spec for _ in arrays],
        out_specs=[spec for _ in plan],
        out_shape=[pltpu.VMEM(shape, jnp.bfloat16) for _ in plan],
        compiler_params=pltpu.CompilerParams(vmem_limit_bytes=4 << 20),
        name="add_blocks",
    )(*[pltpu.with_memory_space_constraint(array, pltpu.VMEM) for array in arrays])


def gather_kernel(place_ref, slot_ref, *refs):
    part_refs, out_ref, sum_ref = refs[:-2], refs[-2], refs[-1]
    groups = len(part_refs)
    capacity = part_refs[0].shape[1]
    owner = place_ref[1]
    sum_ref[...] = jnp.zeros(sum_ref.shape, jnp.float32)
    for n, part_ref in enumerate(part_refs):
        for c in range(capacity):
            slot = slot_ref[((owner ^ n) * groups + owner) * capacity + c]
            sum_ref[slot] += part_ref[0, c].astype(jnp.float32)
    for k in range(OWN):
        out_ref[pl.ds(k * ROWS, ROWS), :] = sum_ref[k].T.astype(jnp.bfloat16)


def gather_tiles(place, slots, parts):
    width = parts[0].shape[2]
    scalars = pl.BlockSpec(memory_space=pltpu.SMEM)
    spec = pl.BlockSpec(memory_space=pltpu.VMEM)
    return pl.pallas_call(
        gather_kernel,
        in_specs=[scalars, scalars] + [spec for _ in parts],
        out_specs=spec,
        scratch_shapes=[pltpu.VMEM((OWN, width, ROWS), jnp.float32)],
        out_shape=jax.ShapeDtypeStruct((OWN * ROWS, width), jnp.bfloat16),
        compiler_params=pltpu.CompilerParams(vmem_limit_bytes=6 << 20),
        name="gather_tiles",
    )(place, slots, *[pltpu.with_memory_space_constraint(part, pltpu.VMEM) for part in parts])


def body(out_grad, pair_cells, weight_codes, head_scale, touch_slots, *, replicas):
    tokens, value = out_grad.shape
    width = value // replicas
    groups = touch_slots.shape[0]
    capacity = touch_slots.shape[2]
    pairs = pair_cells.shape[1] * pair_cells.shape[2]
    place = jnp.stack([lax.axis_index("dp"), lax.axis_index("table")]).astype(jnp.int32)
    by_pair = lambda array: array.transpose(1, 2, 0).reshape(pairs, tokens)

    def swap(array, axis, bit):
        return lax.ppermute(array, axis, [(i, i ^ bit) for i in range(lax.axis_size(axis))])

    chunks = min(CHUNKS, groups)
    size = groups // chunks
    edges = sorted({max(edge and 1, edge * chunks // CHUNKS) for edge in EDGES})
    pieces = [{m: [] for m in range(0, replicas, 2)} for _ in range(chunks)]
    sent = None
    for stage, (first, stop) in enumerate(zip(edges, edges[1:])):
        if stage == 0:
            coef, flip, *outs = first_products(
                place,
                head_scale,
                by_pair(pair_cells),
                by_pair(weight_codes),
                out_grad,
                replicas,
                width,
                capacity,
                groups,
                stop * size,
            )
        else:
            outs = rest_products(place, coef, flip, sent, replicas, width, capacity, groups, first * size, stop * size)
        for m in sorted(range(replicas), reverse=True):
            array = swap(outs[m], "dp", 1) if m & 1 else outs[m]
            for n in range(first, stop):
                pieces[n][m & ~1].append((array, n - first))
        some = pieces[first:stop]
        sent = outs[0]
        bit = 2
        while bit < replicas:
            masks = [m for m in sorted(some[0], reverse=True) if m & bit]
            sums = add_blocks([piece.pop(m) for piece in some for m in masks], size)
            sent = sums[0] if bit == 2 else sent
            sums = iter(sums)
            for n, piece in enumerate(some, first):
                for m in masks:
                    piece[m ^ bit].append((swap(next(sums), "dp", bit), 0))
            bit *= 2
    parts = {}
    for chunk, piece in enumerate(pieces):
        (mine,) = add_blocks([piece[0]], size)
        for i in range(size):
            distance = distance_at(chunk * size + i, groups)
            part = mine if size == 1 else mine[i : i + 1]
            parts[distance] = swap(part, "table", distance) if distance else part
    return gather_tiles(place, touch_slots.reshape(-1), [parts[n] for n in range(groups)])


def solution(mesh):
    return jax.shard_map(
        functools.partial(body, replicas=mesh.shape["dp"]),
        mesh=mesh,
        in_specs=(
            P(("dp", "table"), None),
            P(("dp", "table"), None, None),
            P(("dp", "table"), None, None),
            P(),
            P(),
        ),
        out_specs=P("table", "dp"),
        check_vma=False,
    )
```

```python
import functools

import jax
import jax.numpy as jnp
from jax import lax
from jax.experimental import pallas as pl
from jax.experimental.pallas import tpu as pltpu
from jax.sharding import PartitionSpec as P


ROWS = 128
TOUCH = 32
OWN = 8
CELL_BITS = 12
CODE_BIAS = 128
BLOCK = 128
SIDE = 64
CHUNK_EDGES = (0, 2, 4, 8, 12, 16, 20, 24, 28, 32)
STAGE_EDGES = (0, 8, 16, 32)
LATE = 3


def fill_coef(scale_ref, cells_ref, codes_ref, write, low_ref, high_ref, weight_ref, table_ref):
    pairs, block = cells_ref.shape
    heads = scale_ref.shape[0]
    packed = (cells_ref[...] | ((codes_ref[...] + CODE_BIAS) << CELL_BITS)).T
    stride = table_ref.shape[0] // TOUCH
    tile = (packed >> 7) & (TOUCH - 1)
    upper = (packed >> 6) & 1
    low_ref[...] = (packed & (SIDE - 1)).astype(jnp.float32)
    high_ref[...] = (tile + TOUCH * upper).astype(jnp.float32)
    head = lax.broadcasted_iota(jnp.int32, (1, pairs), 1) // (pairs // heads)
    scale = jnp.zeros((1, pairs), jnp.float32)
    for h in range(heads):
        scale = jnp.where(head == h, scale_ref[h] / 128.0, scale)
    weight_ref[...] = ((packed >> CELL_BITS) - CODE_BIAS).astype(jnp.float32) * scale
    iota = lax.broadcasted_iota(jnp.int32, (SIDE, pairs), 0).astype(jnp.float32).astype(jnp.bfloat16)

    def spread(ref, token):
        row = jnp.broadcast_to(ref[pl.ds(token, 1), :], (16, pairs)).astype(jnp.bfloat16)
        return jnp.concatenate([row] * (SIDE // 16), axis=0)

    for token in range(block):
        low_hot = jnp.where(spread(low_ref, token) == iota, jnp.bfloat16(1), jnp.bfloat16(0))
        high_hot = jnp.where(spread(high_ref, token) == iota, spread(weight_ref, token), jnp.bfloat16(0))
        table = lax.dot_general(
            high_hot, low_hot, (((1,), (1,)), ((), ())), preferred_element_type=jnp.float32
        )
        table = jnp.concatenate([table[:TOUCH], table[TOUCH:]], axis=1)
        table_ref[pl.ds(token, TOUCH, stride=stride), :] = table
    for j in range(TOUCH):
        write(j, table_ref[pl.ds(j * stride, block), :].astype(jnp.bfloat16))


def distances(groups):
    half = groups // 2
    far, near = list(range(half, groups)), list(range(half - 1, -1, -1))
    return [far[0], near[0], far[1], near[1]] + far[2:] + near[2:] if half > 2 else far + near


def put_products(flip, coef, out_refs):
    product = jnp.dot(flip, coef, preferred_element_type=jnp.float32)
    for n, out_ref in enumerate(out_refs):
        width = out_ref.shape[1]
        for c in range(out_ref.shape[0]):
            part = product[n * width : (n + 1) * width, c * ROWS : (c + 1) * ROWS]
            out_ref[c] = part.astype(jnp.bfloat16)


def first_kernel(place_ref, scale_ref, cells_ref, codes_ref, *refs, groups):
    replicas = (len(refs) - 9) // 2
    grad_refs, (coef_hbm, flip_hbm), out_refs = refs[:replicas], refs[replicas : replicas + 2], refs[replicas + 2 : -7]
    low_ref, high_ref, weight_ref, table_ref, coef_ref, flip_ref, semaphores = refs[-7:]
    step = pl.program_id(0)
    block = cells_ref.shape[1]
    width = grad_refs[0].shape[1]
    blocks = coef_ref.shape[0] // block
    span = coef_ref.shape[1] // groups

    saves = [
        pltpu.make_async_copy(coef_ref, coef_hbm, semaphores.at[0]),
        pltpu.make_async_copy(flip_ref, flip_hbm, semaphores.at[1]),
    ]

    @pl.when(step < blocks)
    def _():
        rows = pl.ds(pl.multiple_of(step * block, block), block)

        def write(j, part):
            coef_ref[rows, j * ROWS : (j + 1) * ROWS] = part

        for n in range(replicas):
            flip_ref[n * width : (n + 1) * width, rows] = grad_refs[n][...].T
        fill_coef(scale_ref, cells_ref, codes_ref, write, low_ref, high_ref, weight_ref, table_ref)

    @pl.when(step >= blocks)
    def _():
        @pl.when(step == blocks)
        def _():
            for copy in saves:
                copy.start()

        owner = place_ref[2 + step - blocks]
        coef = coef_ref[:, pl.ds(pl.multiple_of(owner * span, span), span)]
        put_products(flip_ref[...], coef, out_refs)

    @pl.when(step == pl.num_programs(0) - 1)
    def _():
        for copy in saves:
            copy.wait()


def first_products(place, head_scale, cells, codes, grads, replicas, width, capacity, groups, length):
    pairs, tokens = cells.shape
    blocks = tokens // BLOCK
    last = blocks - 1
    spec = pl.BlockSpec((pairs, BLOCK), lambda i, *_: (0, jnp.minimum(i, last)))
    outs = [jax.ShapeDtypeStruct((length * capacity, width, ROWS), jnp.bfloat16) for _ in range(replicas)]
    cells_all = TOUCH * ROWS
    return pl.pallas_call(
        functools.partial(first_kernel, groups=groups),
        grid_spec=pltpu.PrefetchScalarGridSpec(
            num_scalar_prefetch=2,
            grid=(blocks + length,),
            in_specs=[spec, spec]
            + [
                pl.BlockSpec((BLOCK, width), lambda i, place, scale, m=m: (jnp.minimum(i, last), place[0] ^ m))
                for m in range(replicas)
            ],
            out_specs=[pl.BlockSpec(memory_space=pl.ANY), pl.BlockSpec(memory_space=pl.ANY)]
            + [
                pl.BlockSpec((capacity, width, ROWS), lambda i, *_: (jnp.maximum(i - blocks, 0), 0, 0))
                for _ in outs
            ],
            scratch_shapes=[
                pltpu.VMEM((BLOCK, pairs), jnp.float32),
                pltpu.VMEM((BLOCK, pairs), jnp.float32),
                pltpu.VMEM((BLOCK, pairs), jnp.float32),
                pltpu.VMEM((TOUCH * (BLOCK + 8), ROWS), jnp.float32),
                pltpu.VMEM((tokens, cells_all), jnp.bfloat16),
                pltpu.VMEM((replicas * width, tokens), jnp.bfloat16),
                pltpu.SemaphoreType.DMA((2,)),
            ],
        ),
        out_shape=[
            jax.ShapeDtypeStruct((tokens, cells_all), jnp.bfloat16),
            jax.ShapeDtypeStruct((replicas * width, tokens), jnp.bfloat16),
        ]
        + outs,
        cost_estimate=pl.CostEstimate(
            flops=2 * tokens * pairs * cells_all * 4, transcendentals=0, bytes_accessed=tokens * cells_all * 4
        ),
        compiler_params=pltpu.CompilerParams(vmem_limit_bytes=26 << 20),
        name="first_products",
    )(place, head_scale, *[pltpu.with_memory_space_constraint(a, pltpu.HBM) for a in [cells, codes] + [grads] * replicas])


def rest_kernel(place_ref, coef_ref, flip_ref, after_ref, *out_refs):
    put_products(flip_ref[...], coef_ref[...], out_refs)


def rest_products(place, coef, flip, after, replicas, width, capacity, first, stop):
    tokens = coef.shape[0]
    length = stop - first
    return pl.pallas_call(
        rest_kernel,
        grid_spec=pltpu.PrefetchScalarGridSpec(
            num_scalar_prefetch=1,
            grid=(length,),
            in_specs=[
                pl.BlockSpec((tokens, capacity * ROWS), lambda i, place: (0, place[2 + first + i])),
                pl.BlockSpec(flip.shape, lambda i, place: (0, 0)),
                pl.BlockSpec(memory_space=pl.ANY),
            ],
            out_specs=[
                pl.BlockSpec((capacity, width, ROWS), lambda i, place: (i, 0, 0)) for _ in range(replicas)
            ],
        ),
        out_shape=[
            jax.ShapeDtypeStruct((length * capacity, width, ROWS), jnp.bfloat16) for _ in range(replicas)
        ],
        cost_estimate=pl.CostEstimate(
            flops=2 * tokens * length * capacity * ROWS * width * replicas,
            transcendentals=0,
            bytes_accessed=2 * length * capacity * ROWS * (tokens + replicas * width) + 2 * replicas * width * tokens,
        ),
        compiler_params=pltpu.CompilerParams(vmem_limit_bytes=16 << 20),
        name="rest_products",
    )(place, coef, flip, after)


def add_kernel(*refs, plan):
    count = len(refs) - len(plan)
    for out_ref, terms in zip(refs[count:], plan):
        total = 0.0
        for n, at in terms:
            total = total + refs[n][at : at + out_ref.shape[0]].astype(jnp.float32)
        out_ref[...] = total.astype(jnp.bfloat16)


def add_tiles(sums, sizes):
    arrays = []
    plan = []
    for terms in sums:
        row = []
        for array, at in terms:
            known = [n for n, other in enumerate(arrays) if other is array]
            if not known:
                known = [len(arrays)]
                arrays.append(array)
            row.append((known[0], at))
        plan.append(tuple(row))
    spec = pl.BlockSpec(memory_space=pltpu.VMEM)
    return pl.pallas_call(
        functools.partial(add_kernel, plan=tuple(plan)),
        in_specs=[spec for _ in arrays],
        out_specs=[spec for _ in plan],
        out_shape=[pltpu.VMEM((size,) + arrays[0].shape[1:], jnp.bfloat16) for size in sizes],
        compiler_params=pltpu.CompilerParams(vmem_limit_bytes=4 << 20),
        name="add_tiles",
    )(*[pltpu.with_memory_space_constraint(array, pltpu.VMEM) for array in arrays])


def gather_kernel(place_ref, slot_ref, *refs, plan, groups, capacity, first, last):
    refs = list(refs)
    sum_ref = refs.pop() if last else refs[-1]
    out_ref = refs.pop()
    owner = place_ref[1]
    if first:
        sum_ref[...] = jnp.zeros(sum_ref.shape, jnp.float32)
    else:
        sum_ref[...] = refs.pop(0)[...]
    for part_ref, (distance, at) in zip(refs, plan):
        for n in range(part_ref.shape[0]):
            slot = slot_ref[((owner ^ distance) * groups + owner) * capacity + at + n]
            sum_ref[slot] += part_ref[n].astype(jnp.float32)
    if last:
        for k in range(OWN):
            out_ref[pl.ds(k * ROWS, ROWS), :] = sum_ref[k].T.astype(jnp.bfloat16)


def gather_tiles(place, slots, parts, groups, capacity, before=None, last=True):
    width = parts[0][2].shape[1]
    scalars = pl.BlockSpec(memory_space=pltpu.SMEM)
    spec = pl.BlockSpec(memory_space=pltpu.VMEM)
    arrays = [array for _, _, array in parts]
    if before is not None:
        arrays.insert(0, before)
    total = pltpu.VMEM((OWN, width, ROWS), jnp.float32)
    return pl.pallas_call(
        functools.partial(
            gather_kernel,
            plan=tuple((distance, at) for distance, at, _ in parts),
            groups=groups,
            capacity=capacity,
            first=before is None,
            last=last,
        ),
        in_specs=[scalars, scalars] + [spec for _ in arrays],
        out_specs=spec,
        scratch_shapes=[total] if last else [],
        out_shape=jax.ShapeDtypeStruct((OWN * ROWS, width), jnp.bfloat16) if last else total,
        compiler_params=pltpu.CompilerParams(vmem_limit_bytes=6 << 20),
        name="gather_tiles",
    )(place, slots, *[pltpu.with_memory_space_constraint(array, pltpu.VMEM) for array in arrays])


def body(out_grad, pair_cells, weight_codes, head_scale, touch_slots, *, replicas):
    tokens, value = out_grad.shape
    width = value // replicas
    groups = touch_slots.shape[0]
    capacity = touch_slots.shape[2]
    pairs = pair_cells.shape[1] * pair_cells.shape[2]
    order = distances(groups)
    owner = lax.axis_index("table")
    place = jnp.stack([lax.axis_index("dp"), owner] + [owner ^ n for n in order]).astype(jnp.int32)
    by_pair = lambda array: array.transpose(1, 2, 0).reshape(pairs, tokens)

    def swap(array, axis, bit):
        return lax.ppermute(array, axis, [(i, i ^ bit) for i in range(lax.axis_size(axis))])

    tiles = groups * capacity
    chunks = [(a * tiles // TOUCH, b * tiles // TOUCH) for a, b in zip(CHUNK_EDGES, CHUNK_EDGES[1:])]
    stages = [(a * tiles // TOUCH, b * tiles // TOUCH) for a, b in zip(STAGE_EDGES, STAGE_EDGES[1:])]
    pieces = [{m: [] for m in range(0, replicas, 2)} for _ in chunks]
    sent = None
    for stage, (first, stop) in enumerate(stages):
        if stage == 0:
            coef, flip, *outs = first_products(
                place,
                head_scale,
                by_pair(pair_cells),
                by_pair(weight_codes),
                out_grad,
                replicas,
                width,
                capacity,
                groups,
                stop // capacity,
            )
        else:
            outs = rest_products(
                place, coef, flip, sent, replicas, width, capacity, first // capacity, stop // capacity
            )
        here = [n for n, (a, b) in enumerate(chunks) if first <= a < stop]
        sizes = [chunks[n][1] - chunks[n][0] for n in here]
        for m in sorted(range(replicas), reverse=True):
            array = swap(outs[m], "dp", 1) if m & 1 else outs[m]
            for n in here:
                pieces[n][m & ~1].append((array, chunks[n][0] - first))
        sent = outs[0]
        bit = 2
        while bit < replicas:
            masks = [m for m in sorted(pieces[here[0]], reverse=True) if m & bit]
            sums = add_tiles(
                [pieces[n].pop(m) for n in here for m in masks], [size for size in sizes for _ in masks]
            )
            sent = sums[0] if bit == 2 else sent
            sums = iter(sums)
            for n in here:
                for m in masks:
                    pieces[n][m ^ bit].append((swap(next(sums), "dp", bit), 0))
            bit *= 2
    parts = []
    for (a, b), piece in zip(chunks, pieces):
        (mine,) = add_tiles([piece[0]], [b - a])
        for start in range(a, b, min(capacity, b - a)):
            stop = min(start + capacity, b)
            distance = order[start // capacity]
            part = mine if stop - start == b - a else mine[start - a : stop - a]
            part = swap(part, "table", distance) if distance else part
            parts.append((distance, start % capacity, part))
    slots = touch_slots.reshape(-1)
    late = len(parts) - LATE
    total = gather_tiles(place, slots, parts[:late], groups, capacity, last=False)
    return gather_tiles(place, slots, parts[late:], groups, capacity, before=total)


def solution(mesh):
    return jax.shard_map(
        functools.partial(body, replicas=mesh.shape["dp"]),
        mesh=mesh,
        in_specs=(
            P(("dp", "table"), None),
            P(("dp", "table"), None, None),
            P(("dp", "table"), None, None),
            P(),
            P(),
        ),
        out_specs=P("table", "dp"),
        check_vma=False,
    )
```

```python
import functools

import jax
import jax.numpy as jnp
from jax import lax
from jax.experimental import pallas as pl
from jax.experimental.pallas import tpu as pltpu
from jax.sharding import PartitionSpec as P


ROWS = 128
TOUCH = 32
OWN = 8
CELL_BITS = 12
CODE_BIAS = 128
BLOCK = 256
HALVES = 2
SIDE = 64
CHUNK_EDGES = (0, 2, 4, 8, 12, 16, 20, 24, 28, 32)
STAGE_EDGES = (0, 12, 20, 32)
LATE = 3


def fill_coef(scale_ref, cells_ref, codes_ref, write, low_ref, high_ref, weight_ref, table_ref):
    pairs, block = cells_ref.shape
    heads = scale_ref.shape[0]
    packed = (cells_ref[...] | ((codes_ref[...] + CODE_BIAS) << CELL_BITS)).T
    stride = table_ref.shape[0] // TOUCH
    tile = (packed >> 7) & (TOUCH - 1)
    upper = (packed >> 6) & 1
    low_ref[...] = (packed & (SIDE - 1)).astype(jnp.float32)
    high_ref[...] = (tile + TOUCH * upper).astype(jnp.float32)
    head = lax.broadcasted_iota(jnp.int32, (1, pairs), 1) // (pairs // heads)
    scale = jnp.zeros((1, pairs), jnp.float32)
    for h in range(heads):
        scale = jnp.where(head == h, scale_ref[h] / 128.0, scale)
    weight_ref[...] = ((packed >> CELL_BITS) - CODE_BIAS).astype(jnp.float32) * scale
    iota = lax.broadcasted_iota(jnp.int32, (SIDE, pairs), 0).astype(jnp.float32).astype(jnp.bfloat16)

    def spread(ref, token):
        row = jnp.broadcast_to(ref[pl.ds(token, 1), :], (16, pairs)).astype(jnp.bfloat16)
        return jnp.concatenate([row] * (SIDE // 16), axis=0)

    for token in range(block):
        low_hot = jnp.where(spread(low_ref, token) == iota, jnp.bfloat16(1), jnp.bfloat16(0))
        high_hot = jnp.where(spread(high_ref, token) == iota, spread(weight_ref, token), jnp.bfloat16(0))
        table = lax.dot_general(
            high_hot, low_hot, (((1,), (1,)), ((), ())), preferred_element_type=jnp.float32
        )
        table = jnp.concatenate([table[:TOUCH], table[TOUCH:]], axis=1)
        table_ref[pl.ds(token, TOUCH, stride=stride), :] = table
    for j in range(TOUCH):
        write(j, table_ref[pl.ds(j * stride, block), :].astype(jnp.bfloat16))


def distances(groups):
    half = groups // 2
    far, near = [n ^ 1 for n in range(half, groups)], list(range(half - 1, -1, -1))
    return far[:2] + near[:1] + far[2:3] + near[1:2] + far[3:] + near[2:]


def put_products(flip, coef, out_refs):
    product = jnp.dot(flip, coef, preferred_element_type=jnp.float32)
    for n, out_ref in enumerate(out_refs):
        width = out_ref.shape[1]
        for c in range(out_ref.shape[0]):
            part = product[n * width : (n + 1) * width, c * ROWS : (c + 1) * ROWS]
            out_ref[c] = part.astype(jnp.bfloat16)


def first_kernel(place_ref, scale_ref, cells_ref, codes_ref, *refs, groups):
    replicas = (len(refs) - 5 - 4 * HALVES) // 2
    grad_refs, (coef_hbm, flip_hbm) = refs[:replicas], refs[replicas : replicas + 2]
    out_refs = refs[replicas + 2 : 2 * replicas + 2]
    work_refs = refs[2 * replicas + 2 : -3]
    coef_ref, flip_ref, semaphores = refs[-3:]
    step = pl.program_id(0)
    block = cells_ref.shape[1]
    width = grad_refs[0].shape[1]
    blocks = coef_ref.shape[0] // block
    span = coef_ref.shape[1] // groups

    saves = [
        pltpu.make_async_copy(coef_ref, coef_hbm, semaphores.at[0]),
        pltpu.make_async_copy(flip_ref, flip_hbm, semaphores.at[1]),
    ]

    @pl.when(step < blocks)
    def _():
        rows = pl.ds(pl.multiple_of(step * block, block), block)
        for n in range(replicas):
            flip_ref[n * width : (n + 1) * width, rows] = grad_refs[n][...].T
        part = block // HALVES
        for half in range(HALVES):
            at = slice(half * part, (half + 1) * part)
            rows_of = pl.ds(pl.multiple_of(step * block + half * part, part), part)

            def write(j, value, rows_of=rows_of):
                coef_ref[rows_of, j * ROWS : (j + 1) * ROWS] = value

            fill_coef(
                scale_ref, cells_ref.at[:, at], codes_ref.at[:, at], write, *work_refs[4 * half : 4 * half + 4]
            )

    @pl.when(step >= blocks)
    def _():
        @pl.when(step == blocks)
        def _():
            for copy in saves:
                copy.start()

        owner = place_ref[2 + step - blocks]
        coef = coef_ref[:, pl.ds(pl.multiple_of(owner * span, span), span)]
        put_products(flip_ref[...], coef, out_refs)

    @pl.when(step == pl.num_programs(0) - 1)
    def _():
        for copy in saves:
            copy.wait()


def first_products(place, head_scale, cells, codes, grads, replicas, width, capacity, groups, length):
    pairs, tokens = cells.shape
    blocks = tokens // BLOCK
    last = blocks - 1
    spec = pl.BlockSpec((pairs, BLOCK), lambda i, *_: (0, jnp.minimum(i, last)))
    outs = [jax.ShapeDtypeStruct((length * capacity, width, ROWS), jnp.bfloat16) for _ in range(replicas)]
    cells_all = TOUCH * ROWS
    return pl.pallas_call(
        functools.partial(first_kernel, groups=groups),
        grid_spec=pltpu.PrefetchScalarGridSpec(
            num_scalar_prefetch=2,
            grid=(blocks + length,),
            in_specs=[spec, spec]
            + [
                pl.BlockSpec((BLOCK, width), lambda i, place, scale, m=m: (jnp.minimum(i, last), place[0] ^ m))
                for m in range(replicas)
            ],
            out_specs=[pl.BlockSpec(memory_space=pl.ANY), pl.BlockSpec(memory_space=pl.ANY)]
            + [
                pl.BlockSpec((capacity, width, ROWS), lambda i, *_: (jnp.maximum(i - blocks, 0), 0, 0))
                for _ in outs
            ],
            scratch_shapes=[
                pltpu.VMEM((BLOCK // HALVES, pairs), jnp.float32),
                pltpu.VMEM((BLOCK // HALVES, pairs), jnp.float32),
                pltpu.VMEM((BLOCK // HALVES, pairs), jnp.float32),
                pltpu.VMEM((TOUCH * (BLOCK // HALVES + 8), ROWS), jnp.float32),
            ]
            * HALVES
            + [
                pltpu.VMEM((tokens, cells_all), jnp.bfloat16),
                pltpu.VMEM((replicas * width, tokens), jnp.bfloat16),
                pltpu.SemaphoreType.DMA((2,)),
            ],
        ),
        out_shape=[
            jax.ShapeDtypeStruct((tokens, cells_all), jnp.bfloat16),
            jax.ShapeDtypeStruct((replicas * width, tokens), jnp.bfloat16),
        ]
        + outs,
        cost_estimate=pl.CostEstimate(
            flops=2 * tokens * pairs * cells_all * 4, transcendentals=0, bytes_accessed=tokens * cells_all * 4
        ),
        compiler_params=pltpu.CompilerParams(vmem_limit_bytes=22 << 20),
        name="first_products",
    )(place, pltpu.with_memory_space_constraint(head_scale, pltpu.HBM), *[pltpu.with_memory_space_constraint(a, pltpu.HBM) for a in [cells, codes] + [grads] * replicas])


def rest_kernel(place_ref, coef_ref, flip_ref, *refs, count):
    put_products(flip_ref[...], coef_ref[...], refs[-count:])


def rest_products(place, coef, flip, after, replicas, width, capacity, first, stop):
    tokens = coef.shape[0]
    length = stop - first
    return pl.pallas_call(
        functools.partial(rest_kernel, count=replicas),
        grid_spec=pltpu.PrefetchScalarGridSpec(
            num_scalar_prefetch=1,
            grid=(length,),
            in_specs=[
                pl.BlockSpec((tokens, capacity * ROWS), lambda i, place: (0, place[2 + first + i])),
                pl.BlockSpec(flip.shape, lambda i, place: (0, 0)),
                pl.BlockSpec(memory_space=pl.ANY),
            ],
            out_specs=[
                pl.BlockSpec((capacity, width, ROWS), lambda i, place: (i, 0, 0)) for _ in range(replicas)
            ],
        ),
        out_shape=[
            jax.ShapeDtypeStruct((length * capacity, width, ROWS), jnp.bfloat16) for _ in range(replicas)
        ],
        cost_estimate=pl.CostEstimate(
            flops=2 * tokens * length * capacity * ROWS * width * replicas,
            transcendentals=0,
            bytes_accessed=2 * length * capacity * ROWS * (tokens + replicas * width) + 2 * replicas * width * tokens,
        ),
        compiler_params=pltpu.CompilerParams(vmem_limit_bytes=12 << 20),
        name="rest_products",
    )(place, *[pltpu.with_memory_space_constraint(a, pltpu.VMEM) for a in (coef, flip)], after)


def add_kernel(*refs, plan):
    count = len(refs) - len(plan)
    for out_ref, terms in zip(refs[count:], plan):
        total = 0.0
        for n, at in terms:
            total = total + refs[n][at : at + out_ref.shape[0]].astype(jnp.float32)
        out_ref[...] = total.astype(jnp.bfloat16)


def add_tiles(sums, sizes):
    arrays = []
    plan = []
    for terms in sums:
        row = []
        for array, at in terms:
            known = [n for n, other in enumerate(arrays) if other is array]
            if not known:
                known = [len(arrays)]
                arrays.append(array)
            row.append((known[0], at))
        plan.append(tuple(row))
    spec = pl.BlockSpec(memory_space=pltpu.VMEM)
    return pl.pallas_call(
        functools.partial(add_kernel, plan=tuple(plan)),
        in_specs=[spec for _ in arrays],
        out_specs=[spec for _ in plan],
        out_shape=[pltpu.VMEM((size,) + arrays[0].shape[1:], jnp.bfloat16) for size in sizes],
        compiler_params=pltpu.CompilerParams(vmem_limit_bytes=4 << 20),
        name="add_tiles",
    )(*[pltpu.with_memory_space_constraint(array, pltpu.VMEM) for array in arrays])


def gather_kernel(place_ref, slot_ref, *refs, plan, first, last):
    refs = list(refs)
    sum_ref = refs.pop() if last else refs[-1]
    out_ref = refs.pop()
    owner = place_ref[1]
    if first:
        sum_ref[...] = jnp.zeros(sum_ref.shape, jnp.float32)
    else:
        sum_ref[...] = refs.pop(0)[...]
    for part_ref, (distance, at) in zip(refs, plan):
        for n in range(part_ref.shape[0]):
            slot = slot_ref[owner ^ distance, at + n, owner]
            sum_ref[slot] += part_ref[n].astype(jnp.float32)
    if last:
        for k in range(OWN):
            out_ref[pl.ds(k * ROWS, ROWS), :] = sum_ref[k].T.astype(jnp.bfloat16)


def gather_tiles(place, slots, parts, before=None, last=True):
    width = parts[0][2].shape[1]
    scalars = pl.BlockSpec(memory_space=pltpu.SMEM)
    spec = pl.BlockSpec(memory_space=pltpu.VMEM)
    arrays = [array for _, _, array in parts]
    if before is not None:
        arrays.insert(0, before)
    total = pltpu.VMEM((OWN, width, ROWS), jnp.float32)
    return pl.pallas_call(
        functools.partial(
            gather_kernel,
            plan=tuple((distance, at) for distance, at, _ in parts),
            first=before is None,
            last=last,
        ),
        in_specs=[scalars, scalars] + [spec for _ in arrays],
        out_specs=spec,
        scratch_shapes=[total] if last else [],
        out_shape=jax.ShapeDtypeStruct((OWN * ROWS, width), jnp.bfloat16) if last else total,
        compiler_params=pltpu.CompilerParams(vmem_limit_bytes=6 << 20),
        name="gather_tiles",
    )(place, slots, *[pltpu.with_memory_space_constraint(array, pltpu.VMEM) for array in arrays])


def body(out_grad, pair_cells, weight_codes, head_scale, touch_slots, *, replicas):
    tokens, value = out_grad.shape
    width = value // replicas
    groups = touch_slots.shape[0]
    capacity = touch_slots.shape[2]
    pairs = pair_cells.shape[1] * pair_cells.shape[2]
    order = distances(groups)
    owner = lax.axis_index("table")
    place = jnp.stack([lax.axis_index("dp"), owner] + [owner ^ n for n in order]).astype(jnp.int32)
    by_pair = lambda array: array.transpose(1, 2, 0).reshape(pairs, tokens)

    def swap(array, axis, bit):
        return lax.ppermute(array, axis, [(i, i ^ bit) for i in range(lax.axis_size(axis))])

    tiles = groups * capacity
    chunks = [(a * tiles // TOUCH, b * tiles // TOUCH) for a, b in zip(CHUNK_EDGES, CHUNK_EDGES[1:])]
    stages = [(a * tiles // TOUCH, b * tiles // TOUCH) for a, b in zip(STAGE_EDGES, STAGE_EDGES[1:])]
    pieces = [{m: [] for m in range(0, replicas, 2)} for _ in chunks]
    slots = touch_slots.transpose(0, 2, 1)
    sent = None
    for stage, (first, stop) in enumerate(stages):
        if stage == 0:
            coef, flip, *outs = first_products(
                place,
                head_scale,
                by_pair(pair_cells),
                by_pair(weight_codes),
                out_grad,
                replicas,
                width,
                capacity,
                groups,
                stop // capacity,
            )
        else:
            outs = rest_products(
                place, coef, flip, sent, replicas, width, capacity, first // capacity, stop // capacity
            )
        here = [n for n, (a, b) in enumerate(chunks) if first <= a < stop]
        sizes = [chunks[n][1] - chunks[n][0] for n in here]
        for m in sorted(range(replicas), reverse=True):
            array = swap(outs[m], "dp", 1) if m & 1 else outs[m]
            for n in here:
                pieces[n][m & ~1].append((array, chunks[n][0] - first))
        sent = outs[0]
        bit = 2
        while bit < replicas:
            masks = [m for m in sorted(pieces[here[0]], reverse=True) if m & bit]
            sums = add_tiles(
                [pieces[n].pop(m) for n in here for m in masks], [size for size in sizes for _ in masks]
            )
            sent = sums[0] if bit == 2 else sent
            sums = iter(sums)
            for n in here:
                for m in masks:
                    pieces[n][m ^ bit].append((swap(next(sums), "dp", bit), 0))
            bit *= 2
    parts = []
    for (a, b), piece in zip(chunks, pieces):
        (mine,) = add_tiles([piece[0]], [b - a])
        for start in range(a, b, min(capacity, b - a)):
            stop = min(start + capacity, b)
            distance = order[start // capacity]
            part = mine if stop - start == b - a else mine[start - a : stop - a]
            part = swap(part, "table", distance) if distance else part
            parts.append((distance, start % capacity, part))
    late = len(parts) - LATE
    total = gather_tiles(place, slots, parts[:late], last=False)
    return gather_tiles(place, slots, parts[late:], before=total)


def solution(mesh):
    return jax.shard_map(
        functools.partial(body, replicas=mesh.shape["dp"]),
        mesh=mesh,
        in_specs=(
            P(("dp", "table"), None),
            P(("dp", "table"), None, None),
            P(("dp", "table"), None, None),
            P(),
            P(),
        ),
        out_specs=P("table", "dp"),
        check_vma=False,
    )
```

```python
import functools

import jax
import jax.numpy as jnp
from jax import lax
from jax.experimental import pallas as pl
from jax.experimental.pallas import tpu as pltpu
from jax.sharding import PartitionSpec as P


ROWS = 128
TOUCH = 32
OWN = 8
CELL_BITS = 12
CODE_BIAS = 128
BLOCK = 256
HALVES = 2
SIDE = 64
CHUNK_EDGES = (0, 2, 4, 8, 12, 16, 20, 24, 28, 32)
STAGE_EDGES = (0, 12, 20, 32)
LATE = 3


def fill_coef(scale_ref, cells_ref, codes_ref, write, low_ref, high_ref, weight_ref, table_ref):
    pairs, block = cells_ref.shape
    heads = scale_ref.shape[0]
    packed = (cells_ref[...] | ((codes_ref[...] + CODE_BIAS) << CELL_BITS)).T
    stride = table_ref.shape[0] // TOUCH
    tile = (packed >> 7) & (TOUCH - 1)
    upper = (packed >> 6) & 1
    low_ref[...] = (packed & (SIDE - 1)).astype(jnp.float32)
    high_ref[...] = (tile + TOUCH * upper).astype(jnp.float32)
    head = lax.broadcasted_iota(jnp.int32, (1, pairs), 1) // (pairs // heads)
    scale = jnp.zeros((1, pairs), jnp.float32)
    for h in range(heads):
        scale = jnp.where(head == h, scale_ref[h] / 128.0, scale)
    weight_ref[...] = ((packed >> CELL_BITS) - CODE_BIAS).astype(jnp.float32) * scale
    iota = lax.broadcasted_iota(jnp.int32, (SIDE, pairs), 0).astype(jnp.float32).astype(jnp.bfloat16)

    def spread(ref, token):
        row = jnp.broadcast_to(ref[pl.ds(token, 1), :], (16, pairs)).astype(jnp.bfloat16)
        return jnp.concatenate([row] * (SIDE // 16), axis=0)

    for token in range(block):
        low_hot = jnp.where(spread(low_ref, token) == iota, jnp.bfloat16(1), jnp.bfloat16(0))
        high_hot = jnp.where(spread(high_ref, token) == iota, spread(weight_ref, token), jnp.bfloat16(0))
        table = lax.dot_general(
            high_hot, low_hot, (((1,), (1,)), ((), ())), preferred_element_type=jnp.float32
        )
        table = jnp.concatenate([table[:TOUCH], table[TOUCH:]], axis=1)
        table_ref[pl.ds(token, TOUCH, stride=stride), :] = table
    for j in range(TOUCH):
        write(j, table_ref[pl.ds(j * stride, block), :].astype(jnp.bfloat16))


def distances(groups):
    half = groups // 2
    far, near = list(range(half, groups)), list(range(half - 1, -1, -1))
    far = far[1:2] + far[:1] + far[2:]
    return far[:3] + [n for n in near if n & 1] + far[3:] + [n for n in near if not n & 1]


def put_products(flip, coef, out_refs):
    product = jnp.dot(flip, coef, preferred_element_type=jnp.float32)
    for n, out_ref in enumerate(out_refs):
        width = out_ref.shape[1]
        for c in range(out_ref.shape[0]):
            part = product[n * width : (n + 1) * width, c * ROWS : (c + 1) * ROWS]
            out_ref[c] = part.astype(jnp.bfloat16)


def first_kernel(place_ref, scale_ref, cells_ref, codes_ref, *refs, groups):
    replicas = (len(refs) - 5 - 4 * HALVES) // 2
    grad_refs, (coef_hbm, flip_hbm) = refs[:replicas], refs[replicas : replicas + 2]
    out_refs = refs[replicas + 2 : 2 * replicas + 2]
    work_refs = refs[2 * replicas + 2 : -3]
    coef_ref, flip_ref, semaphores = refs[-3:]
    step = pl.program_id(0)
    block = cells_ref.shape[1]
    width = grad_refs[0].shape[1]
    blocks = coef_ref.shape[0] // block
    span = coef_ref.shape[1] // groups

    saves = [
        pltpu.make_async_copy(coef_ref, coef_hbm, semaphores.at[0]),
        pltpu.make_async_copy(flip_ref, flip_hbm, semaphores.at[1]),
    ]

    @pl.when(step < blocks)
    def _():
        rows = pl.ds(pl.multiple_of(step * block, block), block)
        for n in range(replicas):
            flip_ref[n * width : (n + 1) * width, rows] = grad_refs[n][...].T
        part = block // HALVES
        for half in range(HALVES):
            at = slice(half * part, (half + 1) * part)
            rows_of = pl.ds(pl.multiple_of(step * block + half * part, part), part)

            def write(j, value, rows_of=rows_of):
                coef_ref[rows_of, j * ROWS : (j + 1) * ROWS] = value

            fill_coef(
                scale_ref, cells_ref.at[:, at], codes_ref.at[:, at], write, *work_refs[4 * half : 4 * half + 4]
            )

    @pl.when(step >= blocks)
    def _():
        @pl.when(step == blocks)
        def _():
            for copy in saves:
                copy.start()

        owner = place_ref[2 + step - blocks]
        coef = coef_ref[:, pl.ds(pl.multiple_of(owner * span, span), span)]
        put_products(flip_ref[...], coef, out_refs)

    @pl.when(step == pl.num_programs(0) - 1)
    def _():
        for copy in saves:
            copy.wait()


def first_products(place, head_scale, cells, codes, grads, replicas, width, capacity, groups, length):
    pairs, tokens = cells.shape
    blocks = tokens // BLOCK
    last = blocks - 1
    spec = pl.BlockSpec((pairs, BLOCK), lambda i, *_: (0, jnp.minimum(i, last)))
    outs = [jax.ShapeDtypeStruct((length * capacity, width, ROWS), jnp.bfloat16) for _ in range(replicas)]
    cells_all = TOUCH * ROWS
    return pl.pallas_call(
        functools.partial(first_kernel, groups=groups),
        grid_spec=pltpu.PrefetchScalarGridSpec(
            num_scalar_prefetch=2,
            grid=(blocks + length,),
            in_specs=[spec, spec]
            + [
                pl.BlockSpec((BLOCK, width), lambda i, place, scale, m=m: (jnp.minimum(i, last), place[0] ^ m))
                for m in range(replicas)
            ],
            out_specs=[pl.BlockSpec(memory_space=pl.ANY), pl.BlockSpec(memory_space=pl.ANY)]
            + [
                pl.BlockSpec((capacity, width, ROWS), lambda i, *_: (jnp.maximum(i - blocks, 0), 0, 0))
                for _ in outs
            ],
            scratch_shapes=[
                pltpu.VMEM((BLOCK // HALVES, pairs), jnp.float32),
                pltpu.VMEM((BLOCK // HALVES, pairs), jnp.float32),
                pltpu.VMEM((BLOCK // HALVES, pairs), jnp.float32),
                pltpu.VMEM((TOUCH * (BLOCK // HALVES + 8), ROWS), jnp.float32),
            ]
            * HALVES
            + [
                pltpu.VMEM((tokens, cells_all), jnp.bfloat16),
                pltpu.VMEM((replicas * width, tokens), jnp.bfloat16),
                pltpu.SemaphoreType.DMA((2,)),
            ],
        ),
        out_shape=[
            jax.ShapeDtypeStruct((tokens, cells_all), jnp.bfloat16),
            jax.ShapeDtypeStruct((replicas * width, tokens), jnp.bfloat16),
        ]
        + outs,
        cost_estimate=pl.CostEstimate(
            flops=2 * tokens * pairs * cells_all * 4, transcendentals=0, bytes_accessed=tokens * cells_all * 4
        ),
        compiler_params=pltpu.CompilerParams(vmem_limit_bytes=22 << 20),
        name="first_products",
    )(place, pltpu.with_memory_space_constraint(head_scale, pltpu.HBM), *[pltpu.with_memory_space_constraint(a, pltpu.HBM) for a in [cells, codes] + [grads] * replicas])


def rest_kernel(place_ref, coef_ref, flip_ref, *refs, count):
    put_products(flip_ref[...], coef_ref[...], refs[-count:])


def rest_products(place, coef, flip, after, replicas, width, capacity, first, stop):
    tokens = coef.shape[0]
    length = stop - first
    return pl.pallas_call(
        functools.partial(rest_kernel, count=replicas),
        grid_spec=pltpu.PrefetchScalarGridSpec(
            num_scalar_prefetch=1,
            grid=(length,),
            in_specs=[
                pl.BlockSpec((tokens, capacity * ROWS), lambda i, place: (0, place[2 + first + i])),
                pl.BlockSpec(flip.shape, lambda i, place: (0, 0)),
                pl.BlockSpec(memory_space=pl.ANY),
            ],
            out_specs=[
                pl.BlockSpec((capacity, width, ROWS), lambda i, place: (i, 0, 0)) for _ in range(replicas)
            ],
        ),
        out_shape=[
            jax.ShapeDtypeStruct((length * capacity, width, ROWS), jnp.bfloat16) for _ in range(replicas)
        ],
        cost_estimate=pl.CostEstimate(
            flops=2 * tokens * length * capacity * ROWS * width * replicas,
            transcendentals=0,
            bytes_accessed=2 * length * capacity * ROWS * (tokens + replicas * width) + 2 * replicas * width * tokens,
        ),
        compiler_params=pltpu.CompilerParams(vmem_limit_bytes=12 << 20),
        name="rest_products",
    )(place, *[pltpu.with_memory_space_constraint(a, pltpu.VMEM) for a in (coef, flip)], after)


def add_kernel(*refs, plan):
    count = len(refs) - len(plan)
    for out_ref, terms in zip(refs[count:], plan):
        total = 0.0
        for n, at in terms:
            total = total + refs[n][at : at + out_ref.shape[0]].astype(jnp.float32)
        out_ref[...] = total.astype(jnp.bfloat16)


def add_tiles(sums, sizes):
    arrays = []
    plan = []
    for terms in sums:
        row = []
        for array, at in terms:
            known = [n for n, other in enumerate(arrays) if other is array]
            if not known:
                known = [len(arrays)]
                arrays.append(array)
            row.append((known[0], at))
        plan.append(tuple(row))
    spec = pl.BlockSpec(memory_space=pltpu.VMEM)
    return pl.pallas_call(
        functools.partial(add_kernel, plan=tuple(plan)),
        in_specs=[spec for _ in arrays],
        out_specs=[spec for _ in plan],
        out_shape=[pltpu.VMEM((size,) + arrays[0].shape[1:], jnp.bfloat16) for size in sizes],
        compiler_params=pltpu.CompilerParams(vmem_limit_bytes=4 << 20),
        name="add_tiles",
    )(*[pltpu.with_memory_space_constraint(array, pltpu.VMEM) for array in arrays])


def gather_kernel(place_ref, slot_ref, *refs, plan, first, last):
    refs = list(refs)
    sum_ref = refs.pop() if last else refs[-1]
    out_ref = refs.pop()
    owner = place_ref[1]
    if first:
        sum_ref[...] = jnp.zeros(sum_ref.shape, jnp.float32)
    else:
        sum_ref[...] = refs.pop(0)[...]
    for part_ref, (distance, at) in zip(refs, plan):
        for n in range(part_ref.shape[0]):
            slot = slot_ref[owner ^ distance, at + n, owner]
            sum_ref[slot] += part_ref[n].astype(jnp.float32)
    if last:
        for k in range(OWN):
            out_ref[pl.ds(k * ROWS, ROWS), :] = sum_ref[k].T.astype(jnp.bfloat16)


def gather_tiles(place, slots, parts, before=None, last=True):
    width = parts[0][2].shape[1]
    scalars = pl.BlockSpec(memory_space=pltpu.SMEM)
    spec = pl.BlockSpec(memory_space=pltpu.VMEM)
    arrays = [array for _, _, array in parts]
    if before is not None:
        arrays.insert(0, before)
    total = pltpu.VMEM((OWN, width, ROWS), jnp.float32)
    return pl.pallas_call(
        functools.partial(
            gather_kernel,
            plan=tuple((distance, at) for distance, at, _ in parts),
            first=before is None,
            last=last,
        ),
        in_specs=[scalars, scalars] + [spec for _ in arrays],
        out_specs=spec,
        scratch_shapes=[total] if last else [],
        out_shape=jax.ShapeDtypeStruct((OWN * ROWS, width), jnp.bfloat16) if last else total,
        compiler_params=pltpu.CompilerParams(vmem_limit_bytes=6 << 20),
        name="gather_tiles",
    )(place, slots, *[pltpu.with_memory_space_constraint(array, pltpu.VMEM) for array in arrays])


def body(out_grad, pair_cells, weight_codes, head_scale, touch_slots, *, replicas):
    tokens, value = out_grad.shape
    width = value // replicas
    groups = touch_slots.shape[0]
    capacity = touch_slots.shape[2]
    pairs = pair_cells.shape[1] * pair_cells.shape[2]
    order = distances(groups)
    owner = lax.axis_index("table")
    place = jnp.stack([lax.axis_index("dp"), owner] + [owner ^ n for n in order]).astype(jnp.int32)
    by_pair = lambda array: array.transpose(1, 2, 0).reshape(pairs, tokens)

    def swap(array, axis, bit):
        return lax.ppermute(array, axis, [(i, i ^ bit) for i in range(lax.axis_size(axis))])

    tiles = groups * capacity
    chunks = [(a * tiles // TOUCH, b * tiles // TOUCH) for a, b in zip(CHUNK_EDGES, CHUNK_EDGES[1:])]
    stages = [(a * tiles // TOUCH, b * tiles // TOUCH) for a, b in zip(STAGE_EDGES, STAGE_EDGES[1:])]
    pieces = [{m: [] for m in range(0, replicas, 2)} for _ in chunks]
    slots = touch_slots.transpose(0, 2, 1)
    sent = None
    for stage, (first, stop) in enumerate(stages):
        if stage == 0:
            coef, flip, *outs = first_products(
                place,
                head_scale,
                by_pair(pair_cells),
                by_pair(weight_codes),
                out_grad,
                replicas,
                width,
                capacity,
                groups,
                stop // capacity,
            )
        else:
            outs = rest_products(
                place, coef, flip, sent, replicas, width, capacity, first // capacity, stop // capacity
            )
        here = [n for n, (a, b) in enumerate(chunks) if first <= a < stop]
        sizes = [chunks[n][1] - chunks[n][0] for n in here]
        for m in sorted(range(replicas), reverse=True):
            array = swap(outs[m], "dp", 1) if m & 1 else outs[m]
            for n in here:
                pieces[n][m & ~1].append((array, chunks[n][0] - first))
        sent = outs[0]
        bit = 2
        while bit < replicas:
            masks = [m for m in sorted(pieces[here[0]], reverse=True) if m & bit]
            sums = add_tiles(
                [pieces[n].pop(m) for n in here for m in masks], [size for size in sizes for _ in masks]
            )
            sent = sums[0] if bit == 2 else sent
            sums = iter(sums)
            for n in here:
                for m in masks:
                    pieces[n][m ^ bit].append((swap(next(sums), "dp", bit), 0))
            bit *= 2
    parts = []
    for (a, b), piece in zip(chunks, pieces):
        (mine,) = add_tiles([piece[0]], [b - a])
        for start in range(a, b, min(capacity, b - a)):
            stop = min(start + capacity, b)
            distance = order[start // capacity]
            part = mine if stop - start == b - a else mine[start - a : stop - a]
            part = swap(part, "table", distance) if distance else part
            parts.append((distance, start % capacity, part))
    late = len(parts) - LATE
    total = gather_tiles(place, slots, parts[:late], last=False)
    return gather_tiles(place, slots, parts[late:], before=total)


def solution(mesh):
    return jax.shard_map(
        functools.partial(body, replicas=mesh.shape["dp"]),
        mesh=mesh,
        in_specs=(
            P(("dp", "table"), None),
            P(("dp", "table"), None, None),
            P(("dp", "table"), None, None),
            P(),
            P(),
        ),
        out_specs=P("table", "dp"),
        check_vma=False,
    )
```

```python
import functools

import jax
import jax.numpy as jnp
from jax import lax
from jax.experimental import pallas as pl
from jax.experimental.pallas import tpu as pltpu
from jax.sharding import PartitionSpec as P


ROWS = 128
TOUCH = 32
OWN = 8
CELL_BITS = 12
CODE_BIAS = 128
BLOCK = 256
HALVES = 2
SIDE = 64
CHUNK_EDGES = (0, 1, 4, 8, 12, 16, 20, 24, 26, 28, 32)
STAGE_EDGES = (0, 12, 20, 32)
LATE = 3


def fill_coef(scale_ref, cells_ref, codes_ref, write, low_ref, high_ref, weight_ref, table_ref):
    pairs, block = cells_ref.shape
    heads = scale_ref.shape[0]
    packed = (cells_ref[...] | ((codes_ref[...] + CODE_BIAS) << CELL_BITS)).T
    stride = table_ref.shape[0] // TOUCH
    tile = (packed >> 7) & (TOUCH - 1)
    upper = (packed >> 6) & 1
    low_ref[...] = (packed & (SIDE - 1)).astype(jnp.float32)
    high_ref[...] = (tile + TOUCH * upper).astype(jnp.float32)
    head = lax.broadcasted_iota(jnp.int32, (1, pairs), 1) // (pairs // heads)
    scale = jnp.zeros((1, pairs), jnp.float32)
    for h in range(heads):
        scale = jnp.where(head == h, scale_ref[h] / 128.0, scale)
    weight_ref[...] = ((packed >> CELL_BITS) - CODE_BIAS).astype(jnp.float32) * scale
    iota = lax.broadcasted_iota(jnp.int32, (SIDE, pairs), 0).astype(jnp.float32).astype(jnp.bfloat16)

    def spread(ref, token):
        row = jnp.broadcast_to(ref[pl.ds(token, 1), :], (16, pairs)).astype(jnp.bfloat16)
        return jnp.concatenate([row] * (SIDE // 16), axis=0)

    for token in range(block):
        low_hot = jnp.where(spread(low_ref, token) == iota, jnp.bfloat16(1), jnp.bfloat16(0))
        high_hot = jnp.where(spread(high_ref, token) == iota, spread(weight_ref, token), jnp.bfloat16(0))
        table = lax.dot_general(
            high_hot, low_hot, (((1,), (1,)), ((), ())), preferred_element_type=jnp.float32
        )
        table = jnp.concatenate([table[:TOUCH], table[TOUCH:]], axis=1)
        table_ref[pl.ds(token, TOUCH, stride=stride), :] = table
    for j in range(TOUCH):
        write(j, table_ref[pl.ds(j * stride, block), :].astype(jnp.bfloat16))


def distances(groups):
    half = groups // 2
    far, near = list(range(half, groups)), list(range(half - 1, -1, -1))
    far = far[1:2] + far[:1] + far[2:]
    return far[:3] + [n for n in near if n & 1] + far[3:] + [n for n in near if not n & 1]


def put_products(flip, coef, out_refs):
    product = jnp.dot(flip, coef, preferred_element_type=jnp.float32)
    for n, out_ref in enumerate(out_refs):
        width = out_ref.shape[1]
        for c in range(out_ref.shape[0]):
            part = product[n * width : (n + 1) * width, c * ROWS : (c + 1) * ROWS]
            out_ref[c] = part.astype(jnp.bfloat16)


def first_kernel(place_ref, scale_ref, cells_ref, codes_ref, *refs, groups):
    replicas = (len(refs) - 5 - 4 * HALVES) // 2
    grad_refs, (coef_hbm, flip_hbm) = refs[:replicas], refs[replicas : replicas + 2]
    out_refs = refs[replicas + 2 : 2 * replicas + 2]
    work_refs = refs[2 * replicas + 2 : -3]
    coef_ref, flip_ref, semaphores = refs[-3:]
    step = pl.program_id(0)
    block = cells_ref.shape[1]
    width = grad_refs[0].shape[1]
    blocks = coef_ref.shape[0] // block
    span = coef_ref.shape[1] // groups

    saves = [
        pltpu.make_async_copy(coef_ref, coef_hbm, semaphores.at[0]),
        pltpu.make_async_copy(flip_ref, flip_hbm, semaphores.at[1]),
    ]

    @pl.when(step < blocks)
    def _():
        rows = pl.ds(pl.multiple_of(step * block, block), block)
        for n in range(replicas):
            flip_ref[n * width : (n + 1) * width, rows] = grad_refs[n][...].T
        part = block // HALVES
        for half in range(HALVES):
            at = slice(half * part, (half + 1) * part)
            rows_of = pl.ds(pl.multiple_of(step * block + half * part, part), part)

            def write(j, value, rows_of=rows_of):
                coef_ref[rows_of, j * ROWS : (j + 1) * ROWS] = value

            fill_coef(
                scale_ref, cells_ref.at[:, at], codes_ref.at[:, at], write, *work_refs[4 * half : 4 * half + 4]
            )

    @pl.when(step >= blocks)
    def _():
        @pl.when(step == blocks)
        def _():
            for copy in saves:
                copy.start()

        owner = place_ref[2 + step - blocks]
        coef = coef_ref[:, pl.ds(pl.multiple_of(owner * span, span), span)]
        put_products(flip_ref[...], coef, out_refs)

    @pl.when(step == pl.num_programs(0) - 1)
    def _():
        for copy in saves:
            copy.wait()


def first_products(place, head_scale, cells, codes, grads, replicas, width, capacity, groups, length):
    pairs, tokens = cells.shape
    blocks = tokens // BLOCK
    last = blocks - 1
    spec = pl.BlockSpec((pairs, BLOCK), lambda i, *_: (0, jnp.minimum(i, last)))
    outs = [jax.ShapeDtypeStruct((length * capacity, width, ROWS), jnp.bfloat16) for _ in range(replicas)]
    cells_all = TOUCH * ROWS
    return pl.pallas_call(
        functools.partial(first_kernel, groups=groups),
        grid_spec=pltpu.PrefetchScalarGridSpec(
            num_scalar_prefetch=2,
            grid=(blocks + length,),
            in_specs=[spec, spec]
            + [
                pl.BlockSpec((BLOCK, width), lambda i, place, scale, m=m: (jnp.minimum(i, last), place[0] ^ m))
                for m in range(replicas)
            ],
            out_specs=[pl.BlockSpec(memory_space=pl.ANY), pl.BlockSpec(memory_space=pl.ANY)]
            + [
                pl.BlockSpec((capacity, width, ROWS), lambda i, *_: (jnp.maximum(i - blocks, 0), 0, 0))
                for _ in outs
            ],
            scratch_shapes=[
                pltpu.VMEM((BLOCK // HALVES, pairs), jnp.float32),
                pltpu.VMEM((BLOCK // HALVES, pairs), jnp.float32),
                pltpu.VMEM((BLOCK // HALVES, pairs), jnp.float32),
                pltpu.VMEM((TOUCH * (BLOCK // HALVES + 8), ROWS), jnp.float32),
            ]
            * HALVES
            + [
                pltpu.VMEM((tokens, cells_all), jnp.bfloat16),
                pltpu.VMEM((replicas * width, tokens), jnp.bfloat16),
                pltpu.SemaphoreType.DMA((2,)),
            ],
        ),
        out_shape=[
            jax.ShapeDtypeStruct((tokens, cells_all), jnp.bfloat16),
            jax.ShapeDtypeStruct((replicas * width, tokens), jnp.bfloat16),
        ]
        + outs,
        cost_estimate=pl.CostEstimate(
            flops=2 * tokens * pairs * cells_all * 4, transcendentals=0, bytes_accessed=tokens * cells_all * 4
        ),
        compiler_params=pltpu.CompilerParams(vmem_limit_bytes=22 << 20),
        name="first_products",
    )(place, pltpu.with_memory_space_constraint(head_scale, pltpu.HBM), *[pltpu.with_memory_space_constraint(a, pltpu.HBM) for a in [cells, codes] + [grads] * replicas])


def rest_kernel(place_ref, coef_ref, flip_ref, *refs, count):
    put_products(flip_ref[...], coef_ref[...], refs[-count:])


def rest_products(place, coef, flip, after, replicas, width, capacity, first, stop):
    tokens = coef.shape[0]
    length = stop - first
    return pl.pallas_call(
        functools.partial(rest_kernel, count=replicas),
        grid_spec=pltpu.PrefetchScalarGridSpec(
            num_scalar_prefetch=1,
            grid=(length,),
            in_specs=[
                pl.BlockSpec((tokens, capacity * ROWS), lambda i, place: (0, place[2 + first + i])),
                pl.BlockSpec(flip.shape, lambda i, place: (0, 0)),
                pl.BlockSpec(memory_space=pl.ANY),
            ],
            out_specs=[
                pl.BlockSpec((capacity, width, ROWS), lambda i, place: (i, 0, 0)) for _ in range(replicas)
            ],
        ),
        out_shape=[
            jax.ShapeDtypeStruct((length * capacity, width, ROWS), jnp.bfloat16) for _ in range(replicas)
        ],
        cost_estimate=pl.CostEstimate(
            flops=2 * tokens * length * capacity * ROWS * width * replicas,
            transcendentals=0,
            bytes_accessed=2 * length * capacity * ROWS * (tokens + replicas * width) + 2 * replicas * width * tokens,
        ),
        compiler_params=pltpu.CompilerParams(vmem_limit_bytes=12 << 20),
        name="rest_products",
    )(place, *[pltpu.with_memory_space_constraint(a, pltpu.VMEM) for a in (coef, flip)], after)


def add_kernel(*refs, plan):
    count = len(refs) - len(plan)
    for out_ref, terms in zip(refs[count:], plan):
        total = 0.0
        for n, at in terms:
            total = total + refs[n][at : at + out_ref.shape[0]].astype(jnp.float32)
        out_ref[...] = total.astype(jnp.bfloat16)


def add_tiles(sums, sizes):
    arrays = []
    plan = []
    for terms in sums:
        row = []
        for array, at in terms:
            known = [n for n, other in enumerate(arrays) if other is array]
            if not known:
                known = [len(arrays)]
                arrays.append(array)
            row.append((known[0], at))
        plan.append(tuple(row))
    spec = pl.BlockSpec(memory_space=pltpu.VMEM)
    return pl.pallas_call(
        functools.partial(add_kernel, plan=tuple(plan)),
        in_specs=[spec for _ in arrays],
        out_specs=[spec for _ in plan],
        out_shape=[pltpu.VMEM((size,) + arrays[0].shape[1:], jnp.bfloat16) for size in sizes],
        compiler_params=pltpu.CompilerParams(vmem_limit_bytes=4 << 20),
        name="add_tiles",
    )(*[pltpu.with_memory_space_constraint(array, pltpu.VMEM) for array in arrays])


def gather_kernel(place_ref, slot_ref, *refs, plan, first, last):
    refs = list(refs)
    sum_ref = refs.pop() if last else refs[-1]
    out_ref = refs.pop()
    owner = place_ref[1]
    if first:
        sum_ref[...] = jnp.zeros(sum_ref.shape, jnp.float32)
    else:
        sum_ref[...] = refs.pop(0)[...]
    for part_ref, (distance, at) in zip(refs, plan):
        for n in range(part_ref.shape[0]):
            slot = slot_ref[owner ^ distance, at + n, owner]
            sum_ref[slot] += part_ref[n].astype(jnp.float32)
    if last:
        for k in range(OWN):
            out_ref[pl.ds(k * ROWS, ROWS), :] = sum_ref[k].T.astype(jnp.bfloat16)


def gather_tiles(place, slots, parts, before=None, last=True):
    width = parts[0][2].shape[1]
    scalars = pl.BlockSpec(memory_space=pltpu.SMEM)
    spec = pl.BlockSpec(memory_space=pltpu.VMEM)
    arrays = [array for _, _, array in parts]
    if before is not None:
        arrays.insert(0, before)
    total = pltpu.VMEM((OWN, width, ROWS), jnp.float32)
    return pl.pallas_call(
        functools.partial(
            gather_kernel,
            plan=tuple((distance, at) for distance, at, _ in parts),
            first=before is None,
            last=last,
        ),
        in_specs=[scalars, scalars] + [spec for _ in arrays],
        out_specs=spec,
        scratch_shapes=[total] if last else [],
        out_shape=jax.ShapeDtypeStruct((OWN * ROWS, width), jnp.bfloat16) if last else total,
        compiler_params=pltpu.CompilerParams(vmem_limit_bytes=6 << 20),
        name="gather_tiles",
    )(place, slots, *[pltpu.with_memory_space_constraint(array, pltpu.VMEM) for array in arrays])


def body(out_grad, pair_cells, weight_codes, head_scale, touch_slots, *, replicas):
    tokens, value = out_grad.shape
    width = value // replicas
    groups = touch_slots.shape[0]
    capacity = touch_slots.shape[2]
    pairs = pair_cells.shape[1] * pair_cells.shape[2]
    order = distances(groups)
    owner = lax.axis_index("table")
    place = jnp.stack([lax.axis_index("dp"), owner] + [owner ^ n for n in order]).astype(jnp.int32)
    by_pair = lambda array: array.transpose(1, 2, 0).reshape(pairs, tokens)

    def swap(array, axis, bit):
        return lax.ppermute(array, axis, [(i, i ^ bit) for i in range(lax.axis_size(axis))])

    tiles = groups * capacity
    chunks = [(a * tiles // TOUCH, b * tiles // TOUCH) for a, b in zip(CHUNK_EDGES, CHUNK_EDGES[1:])]
    stages = [(a * tiles // TOUCH, b * tiles // TOUCH) for a, b in zip(STAGE_EDGES, STAGE_EDGES[1:])]
    pieces = [{m: [] for m in range(0, replicas, 2)} for _ in chunks]
    slots = touch_slots.transpose(0, 2, 1)
    sent = None
    for stage, (first, stop) in enumerate(stages):
        if stage == 0:
            coef, flip, *outs = first_products(
                place,
                head_scale,
                by_pair(pair_cells),
                by_pair(weight_codes),
                out_grad,
                replicas,
                width,
                capacity,
                groups,
                stop // capacity,
            )
        else:
            outs = rest_products(
                place, coef, flip, sent, replicas, width, capacity, first // capacity, stop // capacity
            )
        here = [n for n, (a, b) in enumerate(chunks) if first <= a < stop]
        sizes = [chunks[n][1] - chunks[n][0] for n in here]
        for m in sorted(range(replicas), reverse=True):
            array = swap(outs[m], "dp", 1) if m & 1 else outs[m]
            for n in here:
                pieces[n][m & ~1].append((array, chunks[n][0] - first))
        sent = outs[0]
        bit = 2
        while bit < replicas:
            masks = [m for m in sorted(pieces[here[0]], reverse=True) if m & bit]
            sums = add_tiles(
                [pieces[n].pop(m) for n in here for m in masks], [size for size in sizes for _ in masks]
            )
            sent = sums[0] if bit == 2 else sent
            sums = iter(sums)
            for n in here:
                for m in masks:
                    pieces[n][m ^ bit].append((swap(next(sums), "dp", bit), 0))
            bit *= 2
    parts = []
    for (a, b), piece in zip(chunks, pieces):
        (mine,) = add_tiles([piece[0]], [b - a])
        for start in range(a, b, min(capacity, b - a)):
            stop = min(start + capacity, b)
            distance = order[start // capacity]
            part = mine if stop - start == b - a else mine[start - a : stop - a]
            part = swap(part, "table", distance) if distance else part
            parts.append((distance, start % capacity, part))
    last = len(parts) - 1
    total = gather_tiles(place, slots, parts[: last - LATE] + parts[last:], last=False)
    return gather_tiles(place, slots, parts[last - LATE : last], before=total)


def solution(mesh):
    return jax.shard_map(
        functools.partial(body, replicas=mesh.shape["dp"]),
        mesh=mesh,
        in_specs=(
            P(("dp", "table"), None),
            P(("dp", "table"), None, None),
            P(("dp", "table"), None, None),
            P(),
            P(),
        ),
        out_specs=P("table", "dp"),
        check_vma=False,
    )
```
